128 devices in a mesh: gx: 8 (over z, core), wa: 16 (over x, y).
Axes of the slice: x: 4, y: 4, z: 4, core: 2. Of those that a mesh axis runs over, the one named last changes fastest.
Arguments:
- positions: float32 [2048, 3, 256], P(('gx', 'wa')), may hold values from 0 to 1
- weights: float32 [2048, 256], P(('gx', 'wa')), may hold values from 0.5 to 2
- block_count: int32 [2048], P(('gx', 'wa')), may hold values from 1 to 256
- send_list: int32 [128, 16, 2], P(('gx', 'wa')), may hold values from 0 to 15
- unit_pair: int32 [128, 32], P(('gx', 'wa')), may hold values from 0 to 31, each once within a row
- unit_live: int32 [128], P(('gx', 'wa')), may hold values from 4 to 32, as said below
Outputs:
- slab_counts: float32 [8, 30, 20], P('gx')
- totals: float32 [30, 20], replicated
The draws below stay inside these ranges and needn't reach their ends.
Inputs may be any that keep to these rules, and one draw needn't show every extreme that they name: `unit_pair`: each row holds every slot number once. `unit_live`: the active units of a device are the first ones of its list; some device has all 32 active.
All inputs are finite; a program needn't handle non-finite values.
Results may differ from the reference program's by a relative error of at most 0.0003.
Values sent between devices are 32-bit elements; how exact they have to be, the bound alone decides.
A program may use at most 64 MiB of HBM per device.

```python
import math
import jax
import jax.numpy as jnp
from jax import lax

BLOCK = 256
SBINS = 30
MUBINS = 20
BLK_DEV = 16
CAP = 2
BLOCKS = 2048
N_GX = 8
N_WA = 16
DEVICES = 128


def draw_unit_live(key, part):
    units = N_WA * CAP
    key_level, key_full = jax.random.split(jax.random.fold_in(key, 7))
    level = jax.random.randint(key_level, (DEVICES,), 0, 4)
    counts = jnp.right_shift(jnp.full((DEVICES,), units, jnp.int32), level.astype(jnp.int32))
    fullest = jax.random.randint(key_full, (), 0, DEVICES)
    return jnp.where(jnp.arange(DEVICES, dtype=jnp.int32) == fullest, jnp.int32(units), counts).astype(jnp.int32)


def draw_positions(key, part):
    key_centre, key_extent, key_offset = jax.random.split(jax.random.fold_in(key, 11), 3)
    centres = 0.35 + 0.3 * jax.random.uniform(key_centre, (BLOCKS, 3, 1), jnp.float32)
    extent = jnp.exp(jax.random.uniform(key_extent, (BLOCKS, 1, 1), jnp.float32, jnp.log(0.03), jnp.log(0.12)))
    offset = jax.random.uniform(key_offset, (BLOCKS, 3, BLOCK), jnp.float32) - 0.5
    return (centres + extent * offset).astype(jnp.float32)


def set_ends(result, stream_key, low, top_value):
    place = [jax.random.randint(jax.random.fold_in(stream_key, axis), (), 0, length) for axis, length in enumerate(result.shape)]
    widest = result.shape.index(max(result.shape))
    next_to = place[:widest] + [(place[widest] + 1) % result.shape[widest]] + place[widest + 1:]
    return result.at[tuple(place)].set(low).at[tuple(next_to)].set(top_value)


def steps_of(own_key, dims, shards, smallest, largest):
    loudness, own = 1.0, jax.random.fold_in(own_key, 6)
    for axis_at, parts in shards:
        steps = jnp.exp(jax.random.uniform(jax.random.fold_in(own, axis_at), (parts,), jnp.float32, smallest / len(shards), largest / len(shards)))
        loudness = loudness * jnp.repeat(steps, dims[axis_at] // parts).reshape([-1 if axis == axis_at else 1 for axis in range(len(dims))])
    return loudness


def setup_inputs(seed: int = 0) -> dict:
    arg_keys = jax.random.split(jax.random.key(seed), 7)
    return {
        "positions": draw_positions(jax.random.fold_in(arg_keys[6], 71), 0),
        "weights": jnp.clip(jnp.exp(math.log(2.0) - 1.3862944 * jax.random.uniform(arg_keys[1], (BLOCKS, BLOCK), jnp.float32) ** steps_of(arg_keys[1], (BLOCKS, BLOCK), ((0, 128),), -0.2, 0.2)), 0.5, 2.0),
        "block_count": set_ends(jax.random.randint(arg_keys[2], (BLOCKS,), 1, BLOCK + 1), jax.random.fold_in(arg_keys[2], 1), 1, BLOCK).astype(jnp.int32),
        "send_list": set_ends(jax.random.randint(arg_keys[3], (DEVICES, N_WA, CAP), 0, BLK_DEV), jax.random.fold_in(arg_keys[3], 1), 0, BLK_DEV - 1).astype(jnp.int32),
        "unit_pair": jax.vmap(lambda own: jax.random.permutation(own, N_WA * CAP))(jax.random.split(arg_keys[4], DEVICES)).reshape((DEVICES, N_WA * CAP)).astype(jnp.int32),
        "unit_live": draw_unit_live(jax.random.fold_in(arg_keys[6], 71), 0),
    }


reach = 0.5
viewer = (0.5, 0.5, -1.5)

def group_counts(a_pos, a_wgt, b_pos, b_wgt):
    step = reach / SBINS
    diff = a_pos[:, :, :, None] - b_pos[:, :, None, :]
    eye_at = jnp.array(viewer, dtype=jnp.float32)[None, :, None, None]
    middle = 0.5 * (a_pos[:, :, :, None] + b_pos[:, :, None, :]) + eye_at
    square = lax.optimization_barrier(jnp.sum(diff * diff, axis=1))
    dist = jnp.sqrt(square)
    along = jnp.abs(lax.optimization_barrier(jnp.sum(diff * middle, axis=1))) / jnp.sqrt(jnp.maximum(square, step * step) * lax.optimization_barrier(jnp.sum(middle * middle, axis=1)))
    s_mid = jnp.arange(SBINS, dtype=jnp.float32) + 0.5
    m_mid = jnp.arange(MUBINS, dtype=jnp.float32) + 0.5
    s_hat = jnp.maximum(0.0, 1.0 - jnp.abs(dist[:, None] / step - s_mid[None, :, None, None]))
    pair_w = a_wgt[:, :, None] * b_wgt[:, None, :]
    m_hat = jnp.maximum(0.0, 1.0 - jnp.abs(along[:, None] * MUBINS - m_mid[None, :, None, None])) * pair_w[:, None]
    s_low = lax.optimization_barrier(s_hat.astype(jnp.bfloat16)).astype(jnp.float32)
    m_low = lax.optimization_barrier(m_hat.astype(jnp.bfloat16)).astype(jnp.float32)
    return jnp.einsum('gkab,gjab->kj', s_low, m_low, precision=lax.Precision.HIGHEST)

def reference(positions, weights, block_count, send_list, unit_pair, unit_live):
    units = N_WA * CAP
    live = jnp.arange(BLOCK, dtype=jnp.int32)[None, :] < block_count[:, None]
    masked = jnp.where(live, weights, jnp.float32(0.0))
    slab_ix = jnp.arange(N_GX, dtype=jnp.int32)[:, None, None, None]
    src_ix = jnp.arange(N_WA, dtype=jnp.int32)[None, None, :, None]
    listed = jnp.transpose(send_list.reshape(N_GX, N_WA, N_WA, CAP), (0, 2, 1, 3))
    own = ((slab_ix * N_WA + src_ix) * BLK_DEV + listed).astype(jnp.int32).reshape(DEVICES, units)
    below = jnp.roll(own.reshape(N_GX, N_WA, units), 1, axis=0).reshape(DEVICES, units)
    partner = jnp.take_along_axis(below, unit_pair, axis=1)
    active = jnp.arange(units, dtype=jnp.int32)[None, :] < unit_live[:, None]

    def device_counts(item):
        ids_a, ids_b, act = item
        a_pos = positions[ids_a].reshape(units // 4, 4, 3, BLOCK)
        b_pos = positions[ids_b].reshape(units // 4, 4, 3, BLOCK)
        a_wgt = jnp.where(act[:, None], masked[ids_a], jnp.float32(0.0)).reshape(units // 4, 4, BLOCK)
        b_wgt = masked[ids_b].reshape(units // 4, 4, BLOCK)

        def accumulate(total, group):
            return (total + group_counts(*group), None)
        start = jnp.zeros((SBINS, MUBINS), jnp.float32)
        total, _ = lax.scan(accumulate, start, (a_pos, a_wgt, b_pos, b_wgt))
        return total
    per_device = lax.map(device_counts, (own, partner, active))
    scale = 10.0 * SBINS * MUBINS / (N_WA * units * BLOCK * BLOCK)
    slab_counts = lax.optimization_barrier(jnp.sum(per_device.reshape(N_GX, N_WA, SBINS, MUBINS), axis=1)) * scale
    totals = lax.optimization_barrier(jnp.sum(slab_counts, axis=0)) / N_GX
    return (slab_counts, totals)
```

```python
import functools

import jax
import jax.numpy as jnp
from jax import lax
from jax.experimental import pallas as pl
from jax.experimental.pallas import tpu as pltpu
from jax.sharding import PartitionSpec as P

SBINS = 30
MUBINS = 20
HS, HM = SBINS // 2, MUBINS // 2
reach = 0.5
viewer = (0.5, 0.5, -1.5)
TILES = 32
f32, bf16, i32 = jnp.float32, jnp.bfloat16, jnp.int32


def hats(at, first, second, half):
    spot = jnp.concatenate([at, at - half], axis=0).astype(bf16)
    first = jnp.concatenate([first, first], axis=0).astype(bf16)
    second = jnp.concatenate([second, second], axis=0).astype(bf16)
    zero = jnp.zeros_like(first)
    before = spot == jnp.asarray(-1, bf16)
    out = []
    for q in range(half):
        here = spot == jnp.asarray(q, bf16)
        out.append(jnp.where(here, first, jnp.where(before, second, zero)))
        before = here
    return out


def tile_hats(cols, lane_at, row):
    def of_a(c):
        return jnp.take_along_axis(cols, jnp.full((8, 128), lane_at + c, i32), axis=1)

    def of_b(c):
        return jnp.broadcast_to(row[c : c + 1, :], (8, 128))

    dx, dy, dz = (of_a(c) - of_b(c) for c in range(3))
    square = dx * dx + dy * dy + dz * dz
    norm_a, norm_b = of_a(3), of_b(3)
    s = square * lax.rsqrt(jnp.maximum(square, 1e-30)) - 0.5
    s_at = jnp.floor(s)
    s_part = s - s_at
    mu = (MUBINS / 2) * jnp.abs(norm_a - norm_b) * lax.rsqrt(
        jnp.maximum(square, 1.0) * (norm_a + norm_b - square)
    ) - 0.5
    mu_at = jnp.floor(mu)
    both = of_a(4) * of_b(4)
    upper = (mu - mu_at) * both
    return hats(s_at, 1.0 - s_part, s_part, HS), hats(mu_at, both - upper, upper, HM)


def count_kernel(units, blocks_ref, out_ref, rows_ref, cols_ref, list_ref, list_smem, acc_ref, sem):
    n_blocks = 2 * units
    scale = SBINS / reach
    groups = n_blocks // 16
    for h in range(2):
        x, y, z, w = (blocks_ref[:, 4 * h + c, :] for c in range(4))
        norm = 0.0
        for c, v in enumerate((x, y, z)):
            rows_ref[pl.ds(h * n_blocks, n_blocks), c, :] = v * scale
            moved = (v + viewer[c]) * scale
            norm = norm + moved * moved
        rows_ref[pl.ds(h * n_blocks, n_blocks), 3, :] = 2.0 * norm
        rows_ref[pl.ds(h * n_blocks, n_blocks), 4, :] = w
        for c in range(5, 8):
            rows_ref[pl.ds(h * n_blocks, n_blocks), c, :] = jnp.zeros_like(w)
    far = 2.0 * sum((v * scale) ** 2 for v in viewer)
    rows_ref[2 * n_blocks] = jnp.where(
        lax.broadcasted_iota(i32, (8, 128), 0) == 3, jnp.float32(far), jnp.float32(0.0)
    )
    for k in range(2 * groups):
        cols_ref[k * 128 : (k + 1) * 128, :] = rows_ref[pl.ds(k * 16, 16)].reshape(128, 128).T

    def live_of(s):
        count = 0.0
        for h in range(2):
            w = blocks_ref[pl.ds(s, units, stride=2), 4 * h + 3, :]
            count = count + jnp.where(w > 0.0, 1.0, 0.0)
        return jnp.broadcast_to(jnp.sum(count, axis=1, keepdims=True), (units, 128))

    n_a, n_b = live_of(0), live_of(1)
    rows_a, rows_b = jnp.ceil(n_a / 8), jnp.ceil(n_b / 8)
    lanes_a, lanes_b = jnp.ceil(n_a / 128), jnp.ceil(n_b / 128)
    turned = jnp.where(rows_b * lanes_a < rows_a * lanes_b, 1.0, 0.0)
    n_lanes = jnp.where(turned > 0.0, lanes_a, lanes_b)
    tiles = jnp.where(turned > 0.0, rows_b, rows_a) * n_lanes
    low = lax.broadcasted_iota(i32, (units, units), 1) < lax.broadcasted_iota(i32, (units, units), 0)
    start = jnp.dot(jnp.where(low, 1.0, 0.0), tiles, preferred_element_type=f32)
    total = jnp.sum(tiles, axis=0, keepdims=True)
    unit = lax.broadcasted_iota(i32, (units, 128), 0).astype(f32)
    pair8 = jnp.floor(unit / 8)
    lane16 = 2.0 * (unit - 8.0 * pair8) + turned
    row_const = pair8 * 16.0
    lane = lax.broadcasted_iota(i32, (units, 128), 1).astype(f32)
    n_list = list_ref.shape[0]
    dummy = jnp.float32(2 * n_blocks)
    list_ref[0] = jnp.broadcast_to(total, (8, 128)).astype(i32)

    def fill(k, carry):
        at = lane + k.astype(f32) * 128.0 - start
        inside = (at >= 0.0) & (at < tiles)
        row = jnp.where(n_lanes > 1.5, jnp.floor(at * 0.5), at)
        part = at - row * n_lanes
        half = jnp.floor(row / 16)
        row_at = half * (16.0 * groups) + row_const + (row - 16.0 * half)
        lane_row = part * n_blocks + 2.0 * unit + (1.0 - turned)
        code = row_at * 4096.0 + lane16 * 256.0 + lane_row
        value = jnp.sum(jnp.where(inside, code - dummy, 0.0), axis=0, keepdims=True) + dummy
        list_ref[k + 1] = jnp.broadcast_to(value, (8, 128)).astype(i32)
        return carry

    lax.fori_loop(0, n_list - 1, fill, 0)
    copy = pltpu.make_async_copy(list_ref.at[:, 0, :], list_smem, sem)
    copy.start()
    acc_ref[...] = jnp.zeros_like(acc_ref)
    copy.wait()
    trips = (list_smem[0, 0] + TILES - 1) // TILES

    def load(trip, t):
        place = trip * TILES + t
        code = list_smem[1 + (place >> 7), place & 127]
        at = pl.multiple_of((code >> 12) * 8, 8)
        return tile_hats(cols_ref[pl.ds(at, 8), :], ((code >> 8) & 15) * 8, rows_ref[code & 255])

    def body(trip, carry):
        total = None
        for p in range(TILES // 2):
            s0, m0 = load(trip, 2 * p)
            s1, m1 = load(trip, 2 * p + 1)
            s = jnp.concatenate([jnp.concatenate(s0, 0), jnp.concatenate(s1, 0)], 1)
            m = jnp.concatenate([jnp.concatenate(m0, 0), jnp.concatenate(m1, 0)], 1)
            r = lax.dot_general(s, m, (((1,), (1,)), ((), ())), preferred_element_type=f32)
            total = r if total is None else total + r
        acc_ref[...] += total
        return carry

    lax.fori_loop(0, trips, body, 0)

    def iota(shape, d):
        return lax.broadcasted_iota(i32, shape, d)

    sm = (16 * HS, 16 * HM)
    kept = jnp.where((iota(sm, 0) & 7) == (iota(sm, 1) & 7), acc_ref[...], 0.0)
    r, c = iota((32, 16 * HS), 0), iota((32, 16 * HS), 1)
    to_s = jnp.where((c >> 4) + HS * ((c >> 3) & 1) == r, 1.0, 0.0)
    r, c = iota((16 * HM, 128), 0), iota((16 * HM, 128), 1)
    to_m = jnp.where((r >> 4) + HM * ((r >> 3) & 1) == c, 1.0, 0.0)
    high = lax.Precision.HIGHEST
    by_s = jnp.dot(to_s, kept, precision=high, preferred_element_type=f32)
    bins = jnp.dot(by_s, to_m, precision=high, preferred_element_type=f32)
    packed = bins[0:8]
    for k in range(1, 4):
        packed = packed + pltpu.roll(bins[8 * k : 8 * k + 8], 32 * k, 1)
    out_ref[...] = packed


def pair_counts(blocks):
    units = blocks.shape[0] // 2
    n_list = 1 + (units * 64 + TILES + 127) // 128
    return pl.pallas_call(
        functools.partial(count_kernel, units),
        out_shape=jax.ShapeDtypeStruct((8, 128), f32),
        in_specs=[pl.BlockSpec(memory_space=pltpu.VMEM)],
        out_specs=pl.BlockSpec(memory_space=pltpu.VMEM),
        scratch_shapes=[
            pltpu.VMEM((4 * units + 1, 8, 128), f32),
            pltpu.VMEM((2 * (units // 8) * 128, 128), f32),
            pltpu.VMEM((n_list, 8, 128), i32),
            pltpu.SMEM((n_list, 128), i32),
            pltpu.VMEM((16 * HS, 16 * HM), f32),
            pltpu.SemaphoreType.DMA,
        ],
    )(blocks)


def unpacked(packed):
    return jnp.moveaxis(packed.reshape(8, 4, 32), 1, 0).reshape(32, 32)[:SBINS, :MUBINS]


def from_everyone(shard, axis):
    count = lax.axis_size(axis)
    return lax.all_to_all(
        jnp.broadcast_to(shard[None], (count, *shard.shape)), axis, 0, 0, tiled=True
    )


def per_device(positions, weights, block_count, send_list, unit_pair, unit_live):
    peers = lax.axis_size("wa")
    per_peer = send_list.shape[2]
    units = peers * per_peer
    live = jnp.arange(256, dtype=jnp.int32)[None, :] < block_count[:, None]
    masked = jnp.where(live, weights, jnp.float32(0.0))
    tiles = jnp.concatenate([positions, masked[:, None]], axis=1)
    tiles = jnp.moveaxis(tiles.reshape(-1, 4, 2, 128), 2, 1).reshape(-1, 8, 128)
    own = lax.all_to_all(
        tiles[send_list[0].reshape(-1)].reshape(peers, per_peer, 8, 128), "wa", 0, 0, tiled=True
    )
    count = lax.axis_size("gx")
    below = lax.ppermute(own, "gx", [(i, (i + 1) % count) for i in range(count)])
    own = own.reshape(units, 8, 128)
    partner = below.reshape(units, 8, 128)[unit_pair[0]]
    active = jnp.arange(units, dtype=jnp.int32) < unit_live[0]
    is_weight = (jnp.arange(8) % 4 == 3)[None, :, None]
    own = jnp.where(is_weight & ~active[:, None, None], jnp.float32(0.0), own)
    pairs = jnp.stack([own, partner], axis=1).reshape(peers, per_peer * 2, 8, 128)
    pairs = jnp.roll(pairs, lax.axis_index("wa"), axis=0)
    dealt = lax.all_to_all(pairs, "wa", 0, 0, tiled=True)
    packed = pair_counts(dealt.reshape(units * 2, 8, 128))
    scale = 10.0 * SBINS * MUBINS / (units * peers * 256 * 256)
    slab = jnp.sum(from_everyone(packed, "wa"), axis=0) * scale
    whole = jnp.sum(from_everyone(slab, "gx"), axis=0) / count
    return (unpacked(slab)[None], unpacked(whole))


def solution(mesh):
    spec = P(("gx", "wa"))
    return jax.shard_map(
        per_device,
        mesh=mesh,
        in_specs=(spec,) * 6,
        out_specs=(P("gx", None, None), P()),
        check_vma=False,
    )
```

```python
import functools

import jax
import jax.numpy as jnp
from jax import lax
from jax.experimental import pallas as pl
from jax.experimental.pallas import tpu as pltpu
from jax.sharding import PartitionSpec as P

SBINS = 30
MUBINS = 20
HS, HM = SBINS // 2, MUBINS // 2
reach = 0.5
viewer = (0.5, 0.5, -1.5)
TILES = 32
f32, bf16, i32 = jnp.float32, jnp.bfloat16, jnp.int32
MESH = pl.DeviceIdType.MESH


def hats(at, first, second, half):
    spot = jnp.concatenate([at, at - half], axis=0).astype(bf16)
    first = jnp.concatenate([first, first], axis=0).astype(bf16)
    second = jnp.concatenate([second, second], axis=0).astype(bf16)
    zero = jnp.zeros_like(first)
    before = spot == jnp.asarray(-1, bf16)
    out = []
    for q in range(half):
        here = spot == jnp.asarray(q, bf16)
        out.append(jnp.where(here, first, jnp.where(before, second, zero)))
        before = here
    return out


def tile_hats(cols, lane_at, row):
    def of_a(c):
        return jnp.take_along_axis(cols, jnp.full((8, 128), lane_at + c, i32), axis=1)

    def of_b(c):
        return jnp.broadcast_to(row[c : c + 1, :], (8, 128))

    dx, dy, dz = (of_a(c) - of_b(c) for c in range(3))
    square = dx * dx + dy * dy + dz * dz
    norm_a, norm_b = of_a(3), of_b(3)
    s = square * lax.rsqrt(jnp.maximum(square, 1e-30)) - 0.5
    s_at = jnp.floor(s)
    s_part = s - s_at
    mu = (MUBINS / 2) * jnp.abs(norm_a - norm_b) * lax.rsqrt(
        jnp.maximum(square, 1.0) * (norm_a + norm_b - square)
    ) - 0.5
    mu_at = jnp.floor(mu)
    both = of_a(4) * of_b(4)
    upper = (mu - mu_at) * both
    return hats(s_at, 1.0 - s_part, s_part, HS), hats(mu_at, both - upper, upper, HM)


def iota(shape, d):
    return lax.broadcasted_iota(i32, shape, d)


def plan(a_weights, b_weights):
    def live(halves):
        count = sum(jnp.where(w > 0.0, 1.0, 0.0) for w in halves)
        return jnp.broadcast_to(jnp.sum(count, axis=1, keepdims=True), count.shape)

    n_a, n_b = live(a_weights), live(b_weights)
    rows_a, rows_b = jnp.ceil(n_a / 8), jnp.ceil(n_b / 8)
    lanes_a, lanes_b = jnp.ceil(n_a / 128), jnp.ceil(n_b / 128)
    turned = jnp.where(rows_b * lanes_a < rows_a * lanes_b, 1.0, 0.0)
    n_lanes = jnp.where(turned > 0.0, lanes_a, lanes_b)
    return turned, n_lanes, jnp.where(turned > 0.0, rows_b, rows_a) * n_lanes


def slot_copy(src, dst, send_sem, recv_sem, device):
    return pltpu.make_async_remote_copy(
        src_ref=src, dst_ref=dst, send_sem=send_sem, recv_sem=recv_sem, device_id=device, device_id_type=MESH
    )


def exchange_kernel(
    n_gx, n_wa, count_ref, list_ref, pair_ref, live_ref, pos_ref, wgt_ref, out_ref,
    home_ref, stage_ref, own_ref, below_ref, partner_ref, deal_ref, send_sems, own_sems, below_sems, deal_sems,
):
    g, w = lax.axis_index("gx"), lax.axis_index("wa")
    above, under = lax.rem(g + 1, n_gx), lax.rem(g + n_gx - 1, n_gx)
    units = 2 * n_wa
    barrier = pltpu.get_barrier_semaphore()

    def greet(o, carry):
        p = lax.rem(w + o, n_wa)
        pl.semaphore_signal(barrier, inc=1, device_id=(under, p), device_id_type=MESH)

        @pl.when(o > 0)
        def _():
            pl.semaphore_signal(barrier, inc=1, device_id=(g, p), device_id_type=MESH)

        return carry

    lax.fori_loop(0, n_wa, greet, 0)

    for b in range(pos_ref.shape[0]):
        for h in range(2):
            at = slice(128 * h, 128 * (h + 1))
            home_ref[b, 4 * h : 4 * h + 3, :] = pos_ref[b, :, at]
            keep = iota((1, 128), 1) + 128 * h < count_ref[b]
            home_ref[b, 4 * h + 3 : 4 * h + 4, :] = jnp.where(keep, wgt_ref[b : b + 1, at], 0.0)
    for q in range(units):
        stage_ref[q] = home_ref[list_ref[0, q // 2, q % 2]]
    pl.semaphore_wait(barrier, 2 * n_wa - 1)

    def own_copy(p, rank):
        return slot_copy(
            stage_ref.at[pl.ds(2 * p, 2)], own_ref.at[pl.ds(2 * rank, 2)], send_sems.at[0, p], own_sems.at[rank], (g, p)
        )

    def below_copy(p, rank):
        return slot_copy(
            stage_ref.at[pl.ds(2 * p, 2)], below_ref.at[pl.ds(2 * rank, 2)], send_sems.at[1, p], below_sems.at[rank], (above, p)
        )

    def send(o, carry):
        p = lax.rem(w + o, n_wa)
        below_copy(p, w).start()

        @pl.when(o > 0)
        def _():
            own_copy(p, w).start()

        return carry

    lax.fori_loop(0, n_wa, send, 0)
    own_ref[pl.ds(2 * w, 2)] = stage_ref[pl.ds(2 * w, 2)]

    def arrive(o, carry):
        p = lax.rem(w + o, n_wa)
        below_copy(p, p).wait_recv()

        @pl.when(o > 0)
        def _():
            own_copy(p, p).wait_recv()

        return carry

    lax.fori_loop(0, n_wa, arrive, 0)
    for u in range(units):
        partner_ref[u] = below_ref[pair_ref[0, u]]

    active = iota((units, 128), 0) < live_ref[0]
    a_rows = [own_ref[:, c, :] for c in range(8)]
    b_rows = [partner_ref[:, c, :] for c in range(8)]
    for c in (3, 7):
        a_rows[c] = jnp.where(active, a_rows[c], 0.0)
    tiles = plan((a_rows[3], a_rows[7]), (b_rows[3], b_rows[7]))[2]
    unit = iota((units, 128), 0).astype(f32)
    key = tiles * units + (units - 1 - unit)
    on_lanes = jnp.sum(jnp.where(iota((units, 128), 0) == iota((units, 128), 1), key, 0.0), axis=0, keepdims=True)
    more = (on_lanes > key) & (iota((units, 128), 1) < units)
    rank = jnp.sum(jnp.where(more, 1.0, 0.0), axis=1, keepdims=True)
    place = jnp.where(rank < n_wa, rank, (units - 1 + n_wa) - rank)
    place = jnp.sum(
        jnp.where(iota((units, units), 0) == iota((units, units), 1), place, 0.0), axis=0, keepdims=True
    )
    choice = jnp.where(iota((units, units), 0).astype(f32) == place, 1.0, 0.0)
    chosen = jnp.dot(
        choice, jnp.concatenate(a_rows + b_rows, axis=1), precision=lax.Precision.HIGHEST, preferred_element_type=f32
    )
    for t in range(2):
        for s in range(2):
            for c in range(8):
                at = (8 * s + c) * 128
                deal_ref[:, 2 * t + s, c, :] = chosen[t * n_wa : (t + 1) * n_wa, at : at + 128]

    def deal_copy(o, p, rank):
        return slot_copy(deal_ref.at[o], out_ref.at[rank], send_sems.at[2, o], deal_sems.at[rank], (g, p))

    def deal(o, carry):
        deal_copy(o, lax.rem(w + o, n_wa), w).start()
        return carry

    lax.fori_loop(1, n_wa, deal, 0)
    out_ref[w] = deal_ref[0]

    def finish(o, carry):
        p = lax.rem(w + o, n_wa)
        deal_copy(o, p, p).wait_recv()
        deal_copy(o, p, p).wait_send()
        own_copy(p, p).wait_send()
        below_copy(p, p).wait_send()
        return carry

    lax.fori_loop(1, n_wa, finish, 0)
    below_copy(w, w).wait_send()


def dealt_blocks(n_gx, n_wa, positions, weights, block_count, send_list, unit_pair, unit_live):
    smem, vmem = pl.BlockSpec(memory_space=pltpu.SMEM), pl.BlockSpec(memory_space=pltpu.VMEM)
    units = 2 * n_wa
    return pl.pallas_call(
        functools.partial(exchange_kernel, n_gx, n_wa),
        out_shape=jax.ShapeDtypeStruct((n_wa, 4, 8, 128), f32),
        in_specs=[smem] * 4 + [vmem] * 2,
        out_specs=vmem,
        scratch_shapes=[
            pltpu.VMEM((positions.shape[0], 8, 128), f32),
            pltpu.VMEM((units, 8, 128), f32),
            pltpu.VMEM((units, 8, 128), f32),
            pltpu.VMEM((units, 8, 128), f32),
            pltpu.VMEM((units, 8, 128), f32),
            pltpu.VMEM((n_wa, 4, 8, 128), f32),
            pltpu.SemaphoreType.DMA((3, n_wa)),
            pltpu.SemaphoreType.DMA((n_wa,)),
            pltpu.SemaphoreType.DMA((n_wa,)),
            pltpu.SemaphoreType.DMA((n_wa,)),
        ],
        compiler_params=pltpu.CompilerParams(collective_id=0, has_side_effects=True),
    )(block_count, send_list, unit_pair, unit_live, positions, weights)


def total_kernel(n_gx, n_wa, scale, in_ref, slab_out, whole_out, wa_ref, gx_ref, slab_ref, send_sems, wa_sems, gx_sems):
    g, w = lax.axis_index("gx"), lax.axis_index("wa")
    barrier = pltpu.get_barrier_semaphore()

    def each(n, me, act):
        def step(o, carry):
            act(lax.rem(me + o, n))
            return carry

        lax.fori_loop(1, n, step, 0)

    each(n_wa, w, lambda p: pl.semaphore_signal(barrier, inc=1, device_id=(g, p), device_id_type=MESH))
    each(n_gx, g, lambda p: pl.semaphore_signal(barrier, inc=1, device_id=(p, w), device_id_type=MESH))
    pl.semaphore_wait(barrier, n_wa + n_gx - 2)

    def wa_copy(p, rank):
        return slot_copy(in_ref, wa_ref.at[rank], send_sems.at[0, p], wa_sems.at[rank], (g, p))

    def gx_copy(p, rank):
        return slot_copy(slab_ref, gx_ref.at[rank], send_sems.at[1, p], gx_sems.at[rank], (p, w))

    each(n_wa, w, lambda p: wa_copy(p, w).start())
    wa_ref[w] = in_ref[...]
    each(n_wa, w, lambda p: wa_copy(p, p).wait_recv())
    slab = jnp.sum(wa_ref[...], axis=0) * scale
    slab_ref[...] = slab
    gx_ref[g] = slab

    def unpack(packed, out):
        for k in range(4):
            rows = min(8, SBINS - 8 * k)
            turned = packed if k == 0 else pltpu.roll(packed, 128 - 32 * k, 1)
            out[8 * k : 8 * k + rows, :] = turned[:rows, :MUBINS]

    each(n_gx, g, lambda p: gx_copy(p, g).start())
    unpack(slab, slab_out.at[0])
    each(n_wa, w, lambda p: wa_copy(p, p).wait_send())
    each(n_gx, g, lambda p: gx_copy(p, p).wait_recv())
    unpack(jnp.sum(gx_ref[...], axis=0) / n_gx, whole_out)
    each(n_gx, g, lambda p: gx_copy(p, p).wait_send())


def totals(n_gx, n_wa, scale, packed):
    vmem = pl.BlockSpec(memory_space=pltpu.VMEM)
    return pl.pallas_call(
        functools.partial(total_kernel, n_gx, n_wa, scale),
        out_shape=(
            jax.ShapeDtypeStruct((1, SBINS, MUBINS), f32),
            jax.ShapeDtypeStruct((SBINS, MUBINS), f32),
        ),
        in_specs=[vmem],
        out_specs=(vmem, vmem),
        scratch_shapes=[
            pltpu.VMEM((n_wa, 8, 128), f32),
            pltpu.VMEM((n_gx, 8, 128), f32),
            pltpu.VMEM((8, 128), f32),
            pltpu.SemaphoreType.DMA((2, n_wa)),
            pltpu.SemaphoreType.DMA((n_wa,)),
            pltpu.SemaphoreType.DMA((n_gx,)),
        ],
        compiler_params=pltpu.CompilerParams(collective_id=1, has_side_effects=True),
    )(packed)


def count_kernel(units, blocks_ref, out_ref, rows_ref, cols_ref, list_ref, list_smem, acc_ref, sem):
    n_blocks = 2 * units
    scale = SBINS / reach
    groups = n_blocks // 16
    for h in range(2):
        x, y, z, w = (blocks_ref[:, 4 * h + c, :] for c in range(4))
        norm = 0.0
        for c, v in enumerate((x, y, z)):
            rows_ref[pl.ds(h * n_blocks, n_blocks), c, :] = v * scale
            moved = (v + viewer[c]) * scale
            norm = norm + moved * moved
        rows_ref[pl.ds(h * n_blocks, n_blocks), 3, :] = 2.0 * norm
        rows_ref[pl.ds(h * n_blocks, n_blocks), 4, :] = w
        for c in range(5, 8):
            rows_ref[pl.ds(h * n_blocks, n_blocks), c, :] = jnp.zeros_like(w)
    far = 2.0 * sum((v * scale) ** 2 for v in viewer)
    rows_ref[2 * n_blocks] = jnp.where(
        lax.broadcasted_iota(i32, (8, 128), 0) == 3, jnp.float32(far), jnp.float32(0.0)
    )
    for k in range(2 * groups):
        cols_ref[k * 128 : (k + 1) * 128, :] = rows_ref[pl.ds(k * 16, 16)].reshape(128, 128).T

    def weights_of(s):
        return [blocks_ref[pl.ds(s, units, stride=2), 4 * h + 3, :] for h in range(2)]

    turned, n_lanes, tiles = plan(weights_of(0), weights_of(1))
    low = lax.broadcasted_iota(i32, (units, units), 1) < lax.broadcasted_iota(i32, (units, units), 0)
    start = jnp.dot(jnp.where(low, 1.0, 0.0), tiles, preferred_element_type=f32)
    total = jnp.sum(tiles, axis=0, keepdims=True)
    unit = lax.broadcasted_iota(i32, (units, 128), 0).astype(f32)
    pair8 = jnp.floor(unit / 8)
    lane16 = 2.0 * (unit - 8.0 * pair8) + turned
    row_const = pair8 * 16.0
    lane = lax.broadcasted_iota(i32, (units, 128), 1).astype(f32)
    n_list = list_ref.shape[0]
    dummy = jnp.float32(2 * n_blocks)
    list_ref[0] = jnp.broadcast_to(total, (8, 128)).astype(i32)

    def fill(k, carry):
        at = lane + k.astype(f32) * 128.0 - start
        inside = (at >= 0.0) & (at < tiles)
        row = jnp.where(n_lanes > 1.5, jnp.floor(at * 0.5), at)
        part = at - row * n_lanes
        half = jnp.floor(row / 16)
        row_at = half * (16.0 * groups) + row_const + (row - 16.0 * half)
        lane_row = part * n_blocks + 2.0 * unit + (1.0 - turned)
        code = row_at * 4096.0 + lane16 * 256.0 + lane_row
        value = jnp.sum(jnp.where(inside, code - dummy, 0.0), axis=0, keepdims=True) + dummy
        list_ref[k + 1] = jnp.broadcast_to(value, (8, 128)).astype(i32)
        return carry

    lax.fori_loop(0, n_list - 1, fill, 0)
    copy = pltpu.make_async_copy(list_ref.at[:, 0, :], list_smem, sem)
    copy.start()
    acc_ref[...] = jnp.zeros_like(acc_ref)
    copy.wait()
    trips = (list_smem[0, 0] + TILES - 1) // TILES

    def load(trip, t):
        place = trip * TILES + t
        code = list_smem[1 + (place >> 7), place & 127]
        at = pl.multiple_of((code >> 12) * 8, 8)
        return tile_hats(cols_ref[pl.ds(at, 8), :], ((code >> 8) & 15) * 8, rows_ref[code & 255])

    def body(trip, carry):
        total = None
        for p in range(TILES // 2):
            s0, m0 = load(trip, 2 * p)
            s1, m1 = load(trip, 2 * p + 1)
            s = jnp.concatenate([jnp.concatenate(s0, 0), jnp.concatenate(s1, 0)], 1)
            m = jnp.concatenate([jnp.concatenate(m0, 0), jnp.concatenate(m1, 0)], 1)
            r = lax.dot_general(s, m, (((1,), (1,)), ((), ())), preferred_element_type=f32)
            total = r if total is None else total + r
        acc_ref[...] += total
        return carry

    lax.fori_loop(0, trips, body, 0)

    sm = (16 * HS, 16 * HM)
    kept = jnp.where((iota(sm, 0) & 7) == (iota(sm, 1) & 7), acc_ref[...], 0.0)
    r, c = iota((32, 16 * HS), 0), iota((32, 16 * HS), 1)
    to_s = jnp.where((c >> 4) + HS * ((c >> 3) & 1) == r, 1.0, 0.0)
    r, c = iota((16 * HM, 128), 0), iota((16 * HM, 128), 1)
    to_m = jnp.where((r >> 4) + HM * ((r >> 3) & 1) == c, 1.0, 0.0)
    high = lax.Precision.HIGHEST
    by_s = jnp.dot(to_s, kept, precision=high, preferred_element_type=f32)
    bins = jnp.dot(by_s, to_m, precision=high, preferred_element_type=f32)
    packed = bins[0:8]
    for k in range(1, 4):
        packed = packed + pltpu.roll(bins[8 * k : 8 * k + 8], 32 * k, 1)
    out_ref[...] = packed


def pair_counts(blocks):
    units = blocks.shape[0] // 2
    n_list = 1 + (units * 64 + TILES + 127) // 128
    return pl.pallas_call(
        functools.partial(count_kernel, units),
        out_shape=jax.ShapeDtypeStruct((8, 128), f32),
        in_specs=[pl.BlockSpec(memory_space=pltpu.VMEM)],
        out_specs=pl.BlockSpec(memory_space=pltpu.VMEM),
        scratch_shapes=[
            pltpu.VMEM((4 * units + 1, 8, 128), f32),
            pltpu.VMEM((2 * (units // 8) * 128, 128), f32),
            pltpu.VMEM((n_list, 8, 128), i32),
            pltpu.SMEM((n_list, 128), i32),
            pltpu.VMEM((16 * HS, 16 * HM), f32),
            pltpu.SemaphoreType.DMA,
        ],
    )(blocks)


def solution(mesh):
    n_gx, n_wa = mesh.shape["gx"], mesh.shape["wa"]
    units = 2 * n_wa
    scale = 10.0 * SBINS * MUBINS / (n_wa * units * 256 * 256)

    def per_device(positions, weights, block_count, send_list, unit_pair, unit_live):
        dealt = dealt_blocks(n_gx, n_wa, positions, weights, block_count, send_list, unit_pair, unit_live)
        packed = pair_counts(dealt.reshape(2 * units, 8, 128))
        return totals(n_gx, n_wa, scale, packed)

    return jax.shard_map(
        per_device,
        mesh=mesh,
        in_specs=(P(("gx", "wa")),) * 6,
        out_specs=(P("gx", None, None), P()),
        check_vma=False,
    )
```

```python
import functools

import jax
import jax.numpy as jnp
from jax import lax
from jax.experimental import pallas as pl
from jax.experimental.pallas import tpu as pltpu
from jax.sharding import PartitionSpec as P

SBINS = 30
MUBINS = 20
HS, HM = SBINS // 2, MUBINS // 2
reach = 0.5
viewer = (0.5, 0.5, -1.5)
TILES = 32
f32, bf16, i32 = jnp.float32, jnp.bfloat16, jnp.int32
MESH = pl.DeviceIdType.MESH


def hats(at, first, second, half):
    spot = jnp.concatenate([at, at - half], axis=0).astype(bf16)
    first = jnp.concatenate([first, first], axis=0).astype(bf16)
    second = jnp.concatenate([second, second], axis=0).astype(bf16)
    zero = jnp.zeros_like(first)
    before = spot == jnp.asarray(-1, bf16)
    out = []
    for q in range(half):
        here = spot == jnp.asarray(q, bf16)
        out.append(jnp.where(here, first, jnp.where(before, second, zero)))
        before = here
    return out


def lane_pick(x, lane):
    numbers = lax.GatherDimensionNumbers(
        offset_dims=(), collapsed_slice_dims=(1,), start_index_map=(1,), operand_batching_dims=(0,), start_indices_batching_dims=(0,)
    )
    return lax.gather(x, lane[..., None], numbers, slice_sizes=(1, 1), mode=lax.GatherScatterMode.PROMISE_IN_BOUNDS)


def tile_hats(cols, lane_at, row):
    def of_a(c):
        return lane_pick(cols, jnp.full((8, 128), lane_at + c, i32))

    def of_b(c):
        return jnp.broadcast_to(row[c : c + 1, :], (8, 128))

    dx, dy, dz = (of_a(c) - of_b(c) for c in range(3))
    square = dx * dx + dy * dy + dz * dz
    norm_a, norm_b = of_a(3), of_b(3)
    s = square * lax.rsqrt(jnp.maximum(square, 1e-30)) - 0.5
    s_at = jnp.floor(s)
    s_part = s - s_at
    mu = (MUBINS / 2) * jnp.abs(norm_a - norm_b) * lax.rsqrt(
        jnp.maximum(square, 1.0) * (norm_a + norm_b - square)
    ) - 0.5
    mu_at = jnp.floor(mu)
    both = of_a(4) * of_b(4)
    upper = (mu - mu_at) * both
    return hats(s_at, 1.0 - s_part, s_part, HS), hats(mu_at, both - upper, upper, HM)


def iota(shape, d):
    return lax.broadcasted_iota(i32, shape, d)


def plan(a_weights, b_weights):
    def live(halves):
        count = sum(jnp.where(w > 0.0, 1.0, 0.0) for w in halves)
        return jnp.broadcast_to(jnp.sum(count, axis=1, keepdims=True), count.shape)

    n_a, n_b = live(a_weights), live(b_weights)
    rows_a, rows_b = jnp.ceil(n_a / 8), jnp.ceil(n_b / 8)
    lanes_a, lanes_b = jnp.ceil(n_a / 128), jnp.ceil(n_b / 128)
    turned = jnp.where(rows_b * lanes_a < rows_a * lanes_b, 1.0, 0.0)
    n_lanes = jnp.where(turned > 0.0, lanes_a, lanes_b)
    return turned, n_lanes, jnp.where(turned > 0.0, rows_b, rows_a) * n_lanes


def slot_copy(src, dst, send_sem, recv_sem, device):
    return pltpu.make_async_remote_copy(
        src_ref=src, dst_ref=dst, send_sem=send_sem, recv_sem=recv_sem, device_id=device, device_id_type=MESH
    )


def exchange_kernel(
    n_gx, n_wa, count_ref, list_ref, pair_ref, live_ref, pos_ref, wgt_ref, out_ref,
    home_ref, stage_ref, own_ref, below_ref, partner_ref, deal_ref, send_sems, own_sems, below_sems, deal_sems,
):
    g, w = lax.axis_index("gx"), lax.axis_index("wa")
    above, under = lax.rem(g + 1, n_gx), lax.rem(g + n_gx - 1, n_gx)
    units = 2 * n_wa
    barrier = pltpu.get_barrier_semaphore()

    def greet(o, carry):
        p = lax.rem(w + o, n_wa)
        pl.semaphore_signal(barrier, inc=1, device_id=(under, p), device_id_type=MESH)

        @pl.when(o > 0)
        def _():
            pl.semaphore_signal(barrier, inc=1, device_id=(g, p), device_id_type=MESH)

        return carry

    lax.fori_loop(0, n_wa, greet, 0)

    for b in range(pos_ref.shape[1]):
        for h in range(2):
            at = slice(128 * h, 128 * (h + 1))
            home_ref[b, 4 * h : 4 * h + 3, :] = pos_ref[:, b, at]
            keep = iota((1, 128), 1) + 128 * h < count_ref[b]
            home_ref[b, 4 * h + 3 : 4 * h + 4, :] = jnp.where(keep, wgt_ref[b : b + 1, at], 0.0)
    for q in range(units):
        stage_ref[q] = home_ref[list_ref[0, q % 2, q // 2]]
    pl.semaphore_wait(barrier, 2 * n_wa - 1)

    def own_copy(p, rank):
        return slot_copy(
            stage_ref.at[pl.ds(2 * p, 2)], own_ref.at[pl.ds(2 * rank, 2)], send_sems.at[0, p], own_sems.at[rank], (g, p)
        )

    def below_copy(p, rank):
        return slot_copy(
            stage_ref.at[pl.ds(2 * p, 2)], below_ref.at[pl.ds(2 * rank, 2)], send_sems.at[1, p], below_sems.at[rank], (above, p)
        )

    def send(o, carry):
        p = lax.rem(w + o, n_wa)
        below_copy(p, w).start()

        @pl.when(o > 0)
        def _():
            own_copy(p, w).start()

        return carry

    lax.fori_loop(0, n_wa, send, 0)
    own_ref[pl.ds(2 * w, 2)] = stage_ref[pl.ds(2 * w, 2)]

    def arrive(o, carry):
        p = lax.rem(w + o, n_wa)
        below_copy(p, p).wait_recv()

        @pl.when(o > 0)
        def _():
            own_copy(p, p).wait_recv()

        return carry

    lax.fori_loop(0, n_wa, arrive, 0)
    for u in range(units):
        partner_ref[u] = below_ref[pair_ref[0, u]]

    active = iota((units, 128), 0) < live_ref[0]
    a_rows = [own_ref[:, c, :] for c in range(8)]
    b_rows = [partner_ref[:, c, :] for c in range(8)]
    for c in (3, 7):
        a_rows[c] = jnp.where(active, a_rows[c], 0.0)
    tiles = plan((a_rows[3], a_rows[7]), (b_rows[3], b_rows[7]))[2]
    unit = iota((units, 128), 0).astype(f32)
    key = tiles * units + (units - 1 - unit)
    on_lanes = jnp.sum(jnp.where(iota((units, 128), 0) == iota((units, 128), 1), key, 0.0), axis=0, keepdims=True)
    more = (on_lanes > key) & (iota((units, 128), 1) < units)
    rank = jnp.sum(jnp.where(more, 1.0, 0.0), axis=1, keepdims=True)
    place = jnp.where(rank < n_wa, rank, (units - 1 + n_wa) - rank)
    place = jnp.sum(
        jnp.where(iota((units, units), 0) == iota((units, units), 1), place, 0.0), axis=0, keepdims=True
    )
    choice = jnp.where(iota((units, units), 0).astype(f32) == place, 1.0, 0.0)
    chosen = jnp.dot(
        choice, jnp.concatenate(a_rows + b_rows, axis=1), precision=lax.Precision.HIGHEST, preferred_element_type=f32
    )
    for t in range(2):
        for s in range(2):
            for c in range(8):
                at = (8 * s + c) * 128
                deal_ref[:, 2 * t + s, c, :] = chosen[t * n_wa : (t + 1) * n_wa, at : at + 128]

    def deal_copy(o, p, rank):
        return slot_copy(deal_ref.at[o], out_ref.at[pl.ds(4 * rank, 4)], send_sems.at[2, o], deal_sems.at[rank], (g, p))

    def deal(o, carry):
        deal_copy(o, lax.rem(w + o, n_wa), w).start()
        return carry

    lax.fori_loop(1, n_wa, deal, 0)
    out_ref[pl.ds(4 * w, 4)] = deal_ref[0]

    def finish(o, carry):
        p = lax.rem(w + o, n_wa)
        deal_copy(o, p, p).wait_recv()
        deal_copy(o, p, p).wait_send()
        own_copy(p, p).wait_send()
        below_copy(p, p).wait_send()
        return carry

    lax.fori_loop(1, n_wa, finish, 0)
    below_copy(w, w).wait_send()


def dealt_blocks(n_gx, n_wa, positions, weights, block_count, send_list, unit_pair, unit_live):
    smem, vmem = pl.BlockSpec(memory_space=pltpu.SMEM), pl.BlockSpec(memory_space=pltpu.VMEM)
    units = 2 * n_wa
    return pl.pallas_call(
        functools.partial(exchange_kernel, n_gx, n_wa),
        out_shape=pltpu.VMEM((2 * units, 8, 128), f32),
        in_specs=[smem] * 4 + [vmem] * 2,
        out_specs=vmem,
        scratch_shapes=[
            pltpu.VMEM((positions.shape[1], 8, 128), f32),
            pltpu.VMEM((units, 8, 128), f32),
            pltpu.VMEM((units, 8, 128), f32),
            pltpu.VMEM((units, 8, 128), f32),
            pltpu.VMEM((units, 8, 128), f32),
            pltpu.VMEM((n_wa, 4, 8, 128), f32),
            pltpu.SemaphoreType.DMA((3, n_wa)),
            pltpu.SemaphoreType.DMA((n_wa,)),
            pltpu.SemaphoreType.DMA((n_wa,)),
            pltpu.SemaphoreType.DMA((n_wa,)),
        ],
        compiler_params=pltpu.CompilerParams(collective_id=0, has_side_effects=True),
    )(block_count, send_list, unit_pair, unit_live, positions, weights)


def total_kernel(n_gx, n_wa, in_ref, slab_out, whole_out, wa_ref, gx_ref, slab_ref, send_sems, wa_sems, gx_sems):
    g, w = lax.axis_index("gx"), lax.axis_index("wa")
    barrier = pltpu.get_barrier_semaphore()

    def each(n, me, act):
        def step(o, carry):
            act(lax.rem(me + o, n))
            return carry

        lax.fori_loop(1, n, step, 0)

    each(n_wa, w, lambda p: pl.semaphore_signal(barrier, inc=1, device_id=(g, p), device_id_type=MESH))
    each(n_gx, g, lambda p: pl.semaphore_signal(barrier, inc=1, device_id=(p, w), device_id_type=MESH))
    pl.semaphore_wait(barrier, n_wa + n_gx - 2)

    def wa_copy(p, rank):
        return slot_copy(in_ref, wa_ref.at[rank], send_sems.at[0, p], wa_sems.at[rank], (g, p))

    def gx_copy(p, rank):
        return slot_copy(slab_ref, gx_ref.at[rank], send_sems.at[1, p], gx_sems.at[rank], (p, w))

    each(n_wa, w, lambda p: wa_copy(p, w).start())
    wa_ref[w] = in_ref[...]
    each(n_wa, w, lambda p: wa_copy(p, p).wait_recv())
    slab = jnp.sum(wa_ref[...], axis=0)
    slab_ref[...] = slab
    gx_ref[g] = slab

    def unpack(packed, out):
        for k in range(3):
            rows = min(8, MUBINS - 8 * k)
            turned = packed if k == 0 else pltpu.roll(packed, 128 - 32 * k, 1)
            out[8 * k : 8 * k + rows, :] = turned[:rows, :SBINS]

    each(n_gx, g, lambda p: gx_copy(p, g).start())
    unpack(slab, slab_out.at[:, 0, :])
    each(n_wa, w, lambda p: wa_copy(p, p).wait_send())
    each(n_gx, g, lambda p: gx_copy(p, p).wait_recv())
    unpack(jnp.sum(gx_ref[...], axis=0), whole_out)
    each(n_gx, g, lambda p: gx_copy(p, p).wait_send())


def totals(n_gx, n_wa, packed):
    vmem = pl.BlockSpec(memory_space=pltpu.VMEM)
    return pl.pallas_call(
        functools.partial(total_kernel, n_gx, n_wa),
        out_shape=(
            pltpu.VMEM((MUBINS, 1, SBINS), f32),
            pltpu.VMEM((MUBINS, SBINS), f32),
        ),
        in_specs=[vmem],
        out_specs=(vmem, vmem),
        scratch_shapes=[
            pltpu.VMEM((n_wa, 8, 128), f32),
            pltpu.VMEM((n_gx, 8, 128), f32),
            pltpu.VMEM((8, 128), f32),
            pltpu.SemaphoreType.DMA((2, n_wa)),
            pltpu.SemaphoreType.DMA((n_wa,)),
            pltpu.SemaphoreType.DMA((n_gx,)),
        ],
        compiler_params=pltpu.CompilerParams(collective_id=1, has_side_effects=True),
    )(packed)


def count_kernel(units, blocks_ref, out_ref, rows_ref, cols_ref, list_ref, list_smem, acc_ref, sem):
    n_blocks = 2 * units
    scale = SBINS / reach
    groups = n_blocks // 16
    for h in range(2):
        x, y, z, w = (blocks_ref[:, 4 * h + c, :] for c in range(4))
        norm = 0.0
        for c, v in enumerate((x, y, z)):
            rows_ref[pl.ds(h * n_blocks, n_blocks), c, :] = v * scale
            moved = (v + viewer[c]) * scale
            norm = norm + moved * moved
        rows_ref[pl.ds(h * n_blocks, n_blocks), 3, :] = 2.0 * norm
        rows_ref[pl.ds(h * n_blocks, n_blocks), 4, :] = w
        for c in range(5, 8):
            rows_ref[pl.ds(h * n_blocks, n_blocks), c, :] = jnp.zeros_like(w)
    far = 2.0 * sum((v * scale) ** 2 for v in viewer)
    rows_ref[2 * n_blocks] = jnp.where(
        lax.broadcasted_iota(i32, (8, 128), 0) == 3, jnp.float32(far), jnp.float32(0.0)
    )
    for k in range(2 * groups):
        cols_ref[k * 128 : (k + 1) * 128, :] = rows_ref[pl.ds(k * 16, 16)].reshape(128, 128).T

    def weights_of(s):
        return [blocks_ref[pl.ds(s, units, stride=2), 4 * h + 3, :] for h in range(2)]

    turned, n_lanes, tiles = plan(weights_of(0), weights_of(1))
    low = lax.broadcasted_iota(i32, (units, units), 1) < lax.broadcasted_iota(i32, (units, units), 0)
    start = jnp.dot(jnp.where(low, 1.0, 0.0), tiles, preferred_element_type=f32)
    total = jnp.sum(tiles, axis=0, keepdims=True)
    unit = lax.broadcasted_iota(i32, (units, 128), 0).astype(f32)
    pair8 = jnp.floor(unit / 8)
    lane16 = 2.0 * (unit - 8.0 * pair8) + turned
    row_const = pair8 * 16.0
    lane = lax.broadcasted_iota(i32, (units, 128), 1).astype(f32)
    n_list = list_ref.shape[0]
    dummy = jnp.float32(2 * n_blocks)
    list_ref[0] = jnp.broadcast_to(total, (8, 128)).astype(i32)

    def fill(k, carry):
        at = lane + k.astype(f32) * 128.0 - start
        inside = (at >= 0.0) & (at < tiles)
        row = jnp.where(n_lanes > 1.5, jnp.floor(at * 0.5), at)
        part = at - row * n_lanes
        half = jnp.floor(row / 16)
        row_at = half * (16.0 * groups) + row_const + (row - 16.0 * half)
        lane_row = part * n_blocks + 2.0 * unit + (1.0 - turned)
        code = row_at * 4096.0 + lane16 * 256.0 + lane_row
        value = jnp.sum(jnp.where(inside, code - dummy, 0.0), axis=0, keepdims=True) + dummy
        list_ref[k + 1] = jnp.broadcast_to(value, (8, 128)).astype(i32)
        return carry

    lax.fori_loop(0, n_list - 1, fill, 0)
    copy = pltpu.make_async_copy(list_ref.at[:, 0, :], list_smem, sem)
    copy.start()
    acc_ref[...] = jnp.zeros_like(acc_ref)
    copy.wait()
    trips = (list_smem[0, 0] + TILES - 1) // TILES

    def load(trip, t):
        place = trip * TILES + t
        code = list_smem[1 + (place >> 7), place & 127]
        at = pl.multiple_of((code >> 12) * 8, 8)
        return tile_hats(cols_ref[pl.ds(at, 8), :], ((code >> 8) & 15) * 8, rows_ref[code & 255])

    def body(trip, carry):
        total = None
        for p in range(TILES // 2):
            s0, m0 = load(trip, 2 * p)
            s1, m1 = load(trip, 2 * p + 1)
            s = jnp.concatenate([jnp.concatenate(s0, 0), jnp.concatenate(s1, 0)], 1)
            m = jnp.concatenate([jnp.concatenate(m0, 0), jnp.concatenate(m1, 0)], 1)
            r = lax.dot_general(s, m, (((1,), (1,)), ((), ())), preferred_element_type=f32)
            total = r if total is None else total + r
        acc_ref[...] += total
        return carry

    lax.fori_loop(0, trips, body, 0)

    sm = (16 * HS, 16 * HM)
    kept = jnp.where((iota(sm, 0) & 7) == (iota(sm, 1) & 7), acc_ref[...], 0.0)
    r, c = iota((32, 16 * HM), 0), iota((32, 16 * HM), 1)
    to_m = jnp.where((c >> 4) + HM * ((c >> 3) & 1) == r, 1.0, 0.0)
    r, c = iota((16 * HS, 128), 0), iota((16 * HS, 128), 1)
    to_s = jnp.where((r >> 4) + HS * ((r >> 3) & 1) == c, 1.0, 0.0)
    high = lax.Precision.HIGHEST
    by_m = lax.dot_general(to_m, kept, (((1,), (1,)), ((), ())), precision=high, preferred_element_type=f32)
    bins = jnp.dot(by_m, to_s, precision=high, preferred_element_type=f32)
    packed = bins[0:8]
    for k in range(1, 3):
        packed = packed + pltpu.roll(bins[8 * k : 8 * k + 8], 32 * k, 1)
    out_ref[...] = packed


def pair_counts(blocks):
    units = blocks.shape[0] // 2
    n_list = 1 + (units * 64 + TILES + 127) // 128
    return pl.pallas_call(
        functools.partial(count_kernel, units),
        out_shape=pltpu.VMEM((8, 128), f32),
        in_specs=[pl.BlockSpec(memory_space=pltpu.VMEM)],
        out_specs=pl.BlockSpec(memory_space=pltpu.VMEM),
        scratch_shapes=[
            pltpu.VMEM((4 * units + 1, 8, 128), f32),
            pltpu.VMEM((2 * (units // 8) * 128, 128), f32),
            pltpu.VMEM((n_list, 8, 128), i32),
            pltpu.SMEM((n_list, 128), i32),
            pltpu.VMEM((16 * HS, 16 * HM), f32),
            pltpu.SemaphoreType.DMA,
        ],
    )(blocks)


def solution(mesh):
    n_gx, n_wa = mesh.shape["gx"], mesh.shape["wa"]
    units = 2 * n_wa
    scale = 10.0 * SBINS * MUBINS / (n_wa * units * 256 * 256)

    def per_device(positions, weights, block_count, send_list, unit_pair, unit_live):
        dealt = dealt_blocks(
            n_gx, n_wa, jnp.transpose(positions, (1, 0, 2)), weights, block_count,
            jnp.transpose(send_list, (0, 2, 1)), unit_pair, unit_live,
        )
        packed = pair_counts(pltpu.with_memory_space_constraint(dealt, pltpu.VMEM))
        slab, whole = totals(n_gx, n_wa, pltpu.with_memory_space_constraint(packed, pltpu.VMEM))
        return jnp.transpose(slab * scale, (1, 2, 0)), (whole * (scale / n_gx)).T

    return jax.shard_map(
        per_device,
        mesh=mesh,
        in_specs=(P(("gx", "wa")),) * 6,
        out_specs=(P("gx", None, None), P()),
        check_vma=False,
    )
```

```python
import functools

import jax
import jax.numpy as jnp
from jax import lax
from jax.experimental import pallas as pl
from jax.experimental.pallas import tpu as pltpu
from jax.sharding import PartitionSpec as P

SBINS = 30
MUBINS = 20
HS, HM = SBINS // 2, MUBINS // 2
reach = 0.5
viewer = (0.5, 0.5, -1.5)
TILES = 32
f32, bf16, i32 = jnp.float32, jnp.bfloat16, jnp.int32
MESH = pl.DeviceIdType.MESH


def hats(at, first, second, half):
    spot = jnp.concatenate([at, at - half], axis=0).astype(bf16)
    first = jnp.concatenate([first, first], axis=0).astype(bf16)
    second = jnp.concatenate([second, second], axis=0).astype(bf16)
    zero = jnp.zeros_like(first)
    before = spot == jnp.asarray(-1, bf16)
    out = []
    for q in range(half):
        here = spot == jnp.asarray(q, bf16)
        out.append(jnp.where(here, first, jnp.where(before, second, zero)))
        before = here
    return out


def lane_pick(x, lane):
    numbers = lax.GatherDimensionNumbers(
        offset_dims=(), collapsed_slice_dims=(1,), start_index_map=(1,), operand_batching_dims=(0,), start_indices_batching_dims=(0,)
    )
    return lax.gather(x, lane[..., None], numbers, slice_sizes=(1, 1), mode=lax.GatherScatterMode.PROMISE_IN_BOUNDS)


def tile_terms(cols, lane_at, row):
    def of_a(c):
        return lane_pick(cols, jnp.full((8, 128), lane_at + c, i32))

    def of_b(c):
        return jnp.broadcast_to(row[c : c + 1, :], (8, 128))

    dx, dy, dz = (of_a(c) - of_b(c) for c in range(3))
    square = dx * dx + dy * dy + dz * dz
    norm_a, norm_b = of_a(3), of_b(3)
    s = square * lax.rsqrt(jnp.maximum(square, 1e-30)) - 0.5
    s_at = jnp.floor(s)
    mu = (MUBINS / 2) * jnp.abs(norm_a - norm_b) * lax.rsqrt(
        jnp.maximum(square, 1.0) * (norm_a + norm_b - square)
    ) - 0.5
    mu_at = jnp.floor(mu)
    both = of_a(4) * of_b(4)
    upper = (mu - mu_at) * both
    return s_at, s - s_at, mu_at, both - upper, upper


def iota(shape, d):
    return lax.broadcasted_iota(i32, shape, d)


def plan(a_weights, b_weights):
    def live(halves):
        count = sum(jnp.where(w > 0.0, 1.0, 0.0) for w in halves)
        return jnp.broadcast_to(jnp.sum(count, axis=1, keepdims=True), count.shape)

    n_a, n_b = live(a_weights), live(b_weights)
    rows_a, rows_b = jnp.ceil(n_a / 8), jnp.ceil(n_b / 8)
    lanes_a, lanes_b = jnp.ceil(n_a / 128), jnp.ceil(n_b / 128)
    turned = jnp.where(rows_b * lanes_a < rows_a * lanes_b, 1.0, 0.0)
    n_lanes = jnp.where(turned > 0.0, lanes_a, lanes_b)
    return turned, n_lanes, jnp.where(turned > 0.0, rows_b, rows_a) * n_lanes


def slot_copy(src, dst, send_sem, recv_sem, device):
    return pltpu.make_async_remote_copy(
        src_ref=src, dst_ref=dst, send_sem=send_sem, recv_sem=recv_sem, device_id=device, device_id_type=MESH
    )


def exchange_kernel(
    n_gx, n_wa, live_ref, count_hbm, list_hbm, pair_hbm, pos_hbm, wgt_hbm, out_ref,
    count_ref, list_ref, pair_ref, pos_ref, wgt_ref, home_ref, stage_ref, own_ref, below_ref, deal_ref,
    load_sems, send_sems, recv_sems,
):
    g, w = lax.axis_index("gx"), lax.axis_index("wa")
    above, under = lax.rem(g + 1, n_gx), lax.rem(g + n_gx - 1, n_gx)
    units = 2 * n_wa
    pairs = ((count_hbm, count_ref), (list_hbm, list_ref), (pair_hbm, pair_ref), (pos_hbm, pos_ref), (wgt_hbm, wgt_ref))
    loads = [pltpu.make_async_copy(src, dst, load_sems.at[k]) for k, (src, dst) in enumerate(pairs)]
    for load in loads:
        load.start()
    barrier = pltpu.get_barrier_semaphore()
    for o in range(n_wa):
        p = lax.rem(w + o, n_wa)
        pl.semaphore_signal(barrier, inc=1, device_id=(under, p), device_id_type=MESH)
        if o:
            pl.semaphore_signal(barrier, inc=1, device_id=(g, p), device_id_type=MESH)
    for load in loads:
        load.wait()

    for b in range(pos_ref.shape[1]):
        for h in range(2):
            at = slice(128 * h, 128 * (h + 1))
            home_ref[b, 4 * h : 4 * h + 3, :] = pos_ref[:, b, at]
            keep = iota((1, 128), 1) + 128 * h < count_ref[b]
            home_ref[b, 4 * h + 3 : 4 * h + 4, :] = jnp.where(keep, wgt_ref[b : b + 1, at], 0.0)
    for q in range(units):
        stage_ref[q] = home_ref[list_ref[0, q % 2, q // 2]]
    pl.semaphore_wait(barrier, 2 * n_wa - 1)

    def two(ref, p):
        return ref.at[pl.ds(2 * p, 2)]

    for o in range(n_wa):
        p = lax.rem(w + o, n_wa)
        slot_copy(two(stage_ref, p), two(below_ref, w), send_sems.at[0], recv_sems.at[0], (above, p)).start()
        if o:
            slot_copy(two(stage_ref, p), two(own_ref, w), send_sems.at[1], recv_sems.at[1], (g, p)).start()
    own_ref[pl.ds(2 * w, 2)] = stage_ref[pl.ds(2 * w, 2)]
    rest = pl.ds(0, units - 2)
    below_all = slot_copy(stage_ref, below_ref, send_sems.at[0], recv_sems.at[0], (above, w))
    own_all = slot_copy(stage_ref.at[rest], own_ref.at[rest], send_sems.at[1], recv_sems.at[1], (above, w))
    below_all.wait_recv()
    own_all.wait_recv()

    active = iota((units, 128), 0) < live_ref[0]
    partner = jnp.concatenate([below_ref[pair_ref[0, u]] for u in range(units)], axis=0)
    row = iota((8 * units, 128), 0)
    dead = ((row & 3) == 3) & ((row >> 3) >= live_ref[0])
    mine = jnp.where(dead, 0.0, own_ref[...].reshape(8 * units, 128))
    three = partner.reshape(units, 8, 128)
    tiles = plan(
        [jnp.where(active, own_ref[:, c, :], 0.0) for c in (3, 7)], [three[:, c, :] for c in (3, 7)]
    )[2]
    unit = iota((units, 128), 0).astype(f32)
    key = tiles * units + (units - 1 - unit)
    on_lanes = jnp.sum(jnp.where(iota((units, 128), 0) == iota((units, 128), 1), key, 0.0), axis=0, keepdims=True)
    more = (on_lanes > key) & (iota((units, 128), 1) < units)
    rank = jnp.sum(jnp.where(more, 1.0, 0.0), axis=1, keepdims=True)
    place = jnp.where(rank < n_wa, rank, (units - 1 + n_wa) - rank)
    wide = (units, 8 * units)
    target = jnp.sum(
        jnp.where(iota(wide, 0) == (iota(wide, 1) >> 3), 8.0 * place + (iota(wide, 1) & 7).astype(f32), 0.0),
        axis=0, keepdims=True,
    )
    square = (8 * units, 8 * units)
    choice = jnp.where(iota(square, 0).astype(f32) == target, 1.0, 0.0).astype(bf16)
    left = jnp.concatenate([mine, partner], axis=1)
    chosen = None
    for _ in range(3):
        part = left.astype(bf16)
        moved = jnp.dot(choice, part, preferred_element_type=f32)
        chosen = moved if chosen is None else chosen + moved
        left = left - part.astype(f32)
    for i in range(units):
        for k in range(2):
            deal_ref[i % n_wa, 2 * (i // n_wa) + k] = chosen[8 * i : 8 * i + 8, 128 * k : 128 * k + 128]

    for o in range(1, n_wa):
        p = lax.rem(w + o, n_wa)
        slot_copy(
            deal_ref.at[o], out_ref.at[pl.ds(4 * w, 4)], send_sems.at[2], recv_sems.at[2], (g, p)
        ).start()
    out_ref[pl.ds(4 * w, 4)] = deal_ref[0]
    below_all.wait_send()
    own_all.wait_send()
    dealt = slot_copy(
        deal_ref.at[pl.ds(1, n_wa - 1)], out_ref.at[pl.ds(0, 4 * (n_wa - 1))], send_sems.at[2], recv_sems.at[2], (above, w)
    )
    dealt.wait_recv()
    dealt.wait_send()


def dealt_blocks(n_gx, n_wa, positions, weights, block_count, send_list, unit_pair, unit_live):
    smem, vmem, anywhere = (pl.BlockSpec(memory_space=m) for m in (pltpu.SMEM, pltpu.VMEM, pl.ANY))
    units = 2 * n_wa
    return pl.pallas_call(
        functools.partial(exchange_kernel, n_gx, n_wa),
        out_shape=pltpu.VMEM((2 * units, 8, 128), f32),
        in_specs=[smem] + [anywhere] * 5,
        out_specs=vmem,
        scratch_shapes=[
            pltpu.SMEM(block_count.shape, i32),
            pltpu.SMEM(send_list.shape, i32),
            pltpu.SMEM(unit_pair.shape, i32),
            pltpu.VMEM(positions.shape, f32),
            pltpu.VMEM(weights.shape, f32),
            pltpu.VMEM((positions.shape[1], 8, 128), f32),
            pltpu.VMEM((units, 8, 128), f32),
            pltpu.VMEM((units, 8, 128), f32),
            pltpu.VMEM((units, 8, 128), f32),
            pltpu.VMEM((n_wa, 4, 8, 128), f32),
            pltpu.SemaphoreType.DMA((5,)),
            pltpu.SemaphoreType.DMA((3,)),
            pltpu.SemaphoreType.DMA((3,)),
        ],
        compiler_params=pltpu.CompilerParams(collective_id=0, has_side_effects=True),
    )(unit_live, block_count, send_list, unit_pair, positions, weights)


def total_kernel(n_gx, n_wa, in_ref, slab_out, whole_out, wa_ref, gx_ref, slab_ref, send_sems, recv_sems):
    g, w = lax.axis_index("gx"), lax.axis_index("wa")
    barrier = pltpu.get_barrier_semaphore()
    wa_peers = [lax.rem(w + o, n_wa) for o in range(1, n_wa)]
    gx_peers = [lax.rem(g + o, n_gx) for o in range(1, n_gx)]
    for p in wa_peers:
        pl.semaphore_signal(barrier, inc=1, device_id=(g, p), device_id_type=MESH)
    for p in gx_peers:
        pl.semaphore_signal(barrier, inc=1, device_id=(p, w), device_id_type=MESH)
    pl.semaphore_wait(barrier, n_wa + n_gx - 2)

    for p in wa_peers:
        slot_copy(in_ref, wa_ref.at[w], send_sems.at[0], recv_sems.at[0], (g, p)).start()
    wa_ref[w] = in_ref[...]
    some = wa_ref.at[pl.ds(0, n_wa - 1)]
    wa_all = slot_copy(some, some, send_sems.at[0], recv_sems.at[0], (lax.rem(g + 1, n_gx), w))
    wa_all.wait_recv()
    slab = jnp.sum(wa_ref[...], axis=0)
    slab_ref[...] = slab
    gx_ref[g] = slab

    def unpack(packed, out):
        for k in range(3):
            rows = min(8, MUBINS - 8 * k)
            turned = packed if k == 0 else pltpu.roll(packed, 128 - 32 * k, 1)
            out[8 * k : 8 * k + rows, :] = turned[:rows, :SBINS]

    for p in gx_peers:
        slot_copy(slab_ref, gx_ref.at[g], send_sems.at[1], recv_sems.at[1], (p, w)).start()
    unpack(slab, slab_out.at[:, 0, :])
    wa_all.wait_send()
    some = gx_ref.at[pl.ds(0, n_gx - 1)]
    gx_all = slot_copy(some, some, send_sems.at[1], recv_sems.at[1], (lax.rem(g + 1, n_gx), w))
    gx_all.wait_recv()
    unpack(jnp.sum(gx_ref[...], axis=0), whole_out)
    gx_all.wait_send()


def totals(n_gx, n_wa, packed):
    vmem = pl.BlockSpec(memory_space=pltpu.VMEM)
    return pl.pallas_call(
        functools.partial(total_kernel, n_gx, n_wa),
        out_shape=(
            pltpu.VMEM((MUBINS, 1, SBINS), f32),
            pltpu.VMEM((MUBINS, SBINS), f32),
        ),
        in_specs=[vmem],
        out_specs=(vmem, vmem),
        scratch_shapes=[
            pltpu.VMEM((n_wa, 8, 128), f32),
            pltpu.VMEM((n_gx, 8, 128), f32),
            pltpu.VMEM((8, 128), f32),
            pltpu.SemaphoreType.DMA((2,)),
            pltpu.SemaphoreType.DMA((2,)),
        ],
        compiler_params=pltpu.CompilerParams(collective_id=1, has_side_effects=True),
    )(packed)


def count_kernel(units, blocks_ref, out_ref, rows_ref, cols_ref, per_unit_ref, list_ref, list_smem, terms_ref, acc_ref, sem):
    n_blocks = 2 * units
    scale = SBINS / reach
    groups = n_blocks // 16

    def weights_of(s):
        return [blocks_ref[pl.ds(s, units, stride=2), 4 * h + 3, :] for h in range(2)]

    turned, n_lanes, tiles = plan(weights_of(0), weights_of(1))
    low = iota((units, units), 1) < iota((units, units), 0)
    start = jnp.dot(jnp.where(low, 1.0, 0.0), tiles, preferred_element_type=f32)
    unit = iota((units, 128), 0).astype(f32)
    eighth = jnp.floor(unit / 8)
    lane16 = 2.0 * (unit - 8.0 * eighth) + turned
    dummy = jnp.float32(2 * n_blocks)
    per_unit_ref[0] = start
    per_unit_ref[1] = start + tiles
    per_unit_ref[2] = jnp.where(n_lanes > 1.5, 0.5, 1.0)
    per_unit_ref[3] = n_lanes
    per_unit_ref[4] = eighth * 65536.0 + lane16 * 256.0 + 2.0 * unit + (1.0 - turned) - dummy
    spot = (iota((8, 128), 0) * 128 + iota((8, 128), 1)).astype(f32)
    n_full = -(-units * 64 // 1024)
    codes = [jnp.full((8, 128), dummy, f32) for _ in range(n_full)]
    for u in range(units):
        first, end, inverse, lanes, base = (jnp.broadcast_to(per_unit_ref[k, u : u + 1, :], (8, 128)) for k in range(5))
        for k in range(n_full):
            place = spot + 1024.0 * k
            at = place - first
            row = jnp.floor(at * inverse)
            code = base + row * 4096.0 + (at - row * lanes) * n_blocks
            code = code + jnp.where(row > 15.5, (groups - 1) * 65536.0, 0.0)
            codes[k] = codes[k] + jnp.where((at >= 0.0) & (place < end), code, 0.0)
    for k in range(n_full):
        list_ref[8 * k : 8 * k + 8, :] = codes[k].astype(i32)
    total = jnp.broadcast_to(jnp.sum(tiles, axis=0, keepdims=True), (8, 128))
    list_ref[8 * n_full : 8 * n_full + 8, :] = jnp.where(iota((8, 128), 0) == 0, dummy, total).astype(i32)
    copy = pltpu.make_async_copy(list_ref, list_smem, sem)
    copy.start()

    at = iota((8, 128), 0)
    eye = sum(jnp.where((at & 3) == c, v, 0.0) for c, v in enumerate(viewer))

    for n in range(n_blocks):
        raw = blocks_ref[n]
        moved = (raw + eye) * scale
        moved = moved * moved
        norm = 2.0 * (moved + pltpu.roll(moved, 7, 0) + pltpu.roll(moved, 6, 0))
        for h in range(2):
            xyz = raw * scale if h == 0 else pltpu.roll(raw * scale, 4, 0)
            weight = pltpu.roll(raw, 1 if h == 0 else 5, 0)
            norms = pltpu.roll(norm, 3 if h == 0 else 7, 0)
            rows_ref[h * n_blocks + n] = jnp.where(at < 3, xyz, jnp.where(at == 3, norms, weight))
    far = 2.0 * sum((v * scale) ** 2 for v in viewer)
    rows_ref[2 * n_blocks] = jnp.where(at == 3, jnp.float32(far), jnp.float32(0.0))
    for k in range(2 * groups):
        cols_ref[k * 128 : (k + 1) * 128, :] = rows_ref[pl.ds(k * 16, 16)].reshape(128, 128).T
    acc_ref[...] = jnp.zeros_like(acc_ref)
    copy.wait()
    trips = (list_smem[8 * n_full + 1, 0] + TILES - 1) // TILES

    def fill(trip):
        for t in range(TILES):
            code = list_smem[trip // (128 // TILES), lax.rem(trip, 128 // TILES) * TILES + t]
            start = pl.multiple_of((code >> 12) * 8, 8)
            terms = tile_terms(cols_ref[pl.ds(start, 8), :], ((code >> 8) & 15) * 8, rows_ref[code & 255])
            for k, v in enumerate(terms):
                terms_ref[t, k] = v

    def both_hats(t):
        s_at, s_part, mu_at, lower, upper = (terms_ref[t, k] for k in range(5))
        return hats(s_at, 1.0 - s_part, s_part, HS), hats(mu_at, lower, upper, HM)

    fill(0)

    def body(trip, carry):
        total = None
        for p in range(TILES // 2):
            s0, m0 = both_hats(2 * p)
            s1, m1 = both_hats(2 * p + 1)
            s = jnp.concatenate([jnp.concatenate(s0, 0), jnp.concatenate(s1, 0)], 1)
            m = jnp.concatenate([jnp.concatenate(m0, 0), jnp.concatenate(m1, 0)], 1)
            r = lax.dot_general(s, m, (((1,), (1,)), ((), ())), preferred_element_type=f32)
            total = r if total is None else total + r
        fill(trip + 1)
        acc_ref[...] += total
        return carry

    lax.fori_loop(0, trips, body, 0)

    sm = (8, 16 * HM)
    same = iota(sm, 0) == (iota(sm, 1) & 7)
    sums = []
    for k in range(SBINS):
        place = 16 * (k % HS) + 8 * (k // HS)
        sums.append(jnp.sum(jnp.where(same, acc_ref[place : place + 8, :], 0.0), axis=0, keepdims=True))
    by_s = jnp.concatenate(sums + [jnp.zeros((128 - SBINS, 16 * HM), f32)], axis=0)
    r, c = iota((32, 16 * HM), 0), iota((32, 16 * HM), 1)
    to_m = jnp.where((c >> 4) + HM * ((c >> 3) & 1) == r, 1.0, 0.0)
    bins = lax.dot_general(
        to_m, by_s, (((1,), (1,)), ((), ())), precision=lax.Precision.HIGHEST, preferred_element_type=f32
    )
    packed = bins[0:8]
    for k in range(1, 3):
        packed = packed + pltpu.roll(bins[8 * k : 8 * k + 8], 32 * k, 1)
    out_ref[...] = packed


def pair_counts(blocks):
    units = blocks.shape[0] // 2
    n_list = 8 * (-(-units * 64 // 1024) + 1)
    return pl.pallas_call(
        functools.partial(count_kernel, units),
        out_shape=pltpu.VMEM((8, 128), f32),
        in_specs=[pl.BlockSpec(memory_space=pltpu.VMEM)],
        out_specs=pl.BlockSpec(memory_space=pltpu.VMEM),
        scratch_shapes=[
            pltpu.VMEM((4 * units + 1, 8, 128), f32),
            pltpu.VMEM((2 * (units // 8) * 128, 128), f32),
            pltpu.VMEM((5, units, 128), f32),
            pltpu.VMEM((n_list, 128), i32),
            pltpu.SMEM((n_list, 128), i32),
            pltpu.VMEM((TILES, 5, 8, 128), f32),
            pltpu.VMEM((16 * HS, 16 * HM), f32),
            pltpu.SemaphoreType.DMA,
        ],
    )(blocks)


def solution(mesh):
    n_gx, n_wa = mesh.shape["gx"], mesh.shape["wa"]
    units = 2 * n_wa
    scale = 10.0 * SBINS * MUBINS / (n_wa * units * 256 * 256)

    def per_device(positions, weights, block_count, send_list, unit_pair, unit_live):
        dealt = dealt_blocks(
            n_gx, n_wa, jnp.transpose(positions, (1, 0, 2)), weights, block_count,
            jnp.transpose(send_list, (0, 2, 1)), unit_pair, unit_live,
        )
        packed = pair_counts(pltpu.with_memory_space_constraint(dealt, pltpu.VMEM))
        slab, whole = totals(n_gx, n_wa, pltpu.with_memory_space_constraint(packed, pltpu.VMEM))
        return jnp.transpose(slab * scale, (1, 2, 0)), (whole * (scale / n_gx)).T

    return jax.shard_map(
        per_device,
        mesh=mesh,
        in_specs=(P(("gx", "wa")),) * 6,
        out_specs=(P("gx", None, None), P()),
        check_vma=False,
    )
```

```python
import functools

import jax
import jax.numpy as jnp
from jax import lax
from jax.experimental import pallas as pl
from jax.experimental.pallas import tpu as pltpu
from jax.sharding import PartitionSpec as P

SBINS = 30
MUBINS = 20
HS, HM = SBINS // 2, MUBINS // 2
reach = 0.5
viewer = (0.5, 0.5, -1.5)
TILES = 48
f32, bf16, i32 = jnp.float32, jnp.bfloat16, jnp.int32
MESH = pl.DeviceIdType.MESH


def hats(at, first, second, half):
    spot = jnp.concatenate([at, at - half], axis=0).astype(bf16)
    first = jnp.concatenate([first, first], axis=0).astype(bf16)
    second = jnp.concatenate([second, second], axis=0).astype(bf16)
    zero = jnp.zeros_like(first)
    before = spot == jnp.asarray(-1, bf16)
    out = []
    for q in range(half):
        here = spot == jnp.asarray(q, bf16)
        out.append(jnp.where(here, first, jnp.where(before, second, zero)))
        before = here
    return out


def lane_pick(x, lane):
    numbers = lax.GatherDimensionNumbers(
        offset_dims=(), collapsed_slice_dims=(1,), start_index_map=(1,), operand_batching_dims=(0,), start_indices_batching_dims=(0,)
    )
    return lax.gather(x, lane[..., None], numbers, slice_sizes=(1, 1), mode=lax.GatherScatterMode.PROMISE_IN_BOUNDS)


def tile_terms(cols, lane_at, row):
    def of_a(c):
        return lane_pick(cols, jnp.full((8, 128), lane_at + c, i32))

    def of_b(c):
        return jnp.broadcast_to(row[c : c + 1, :], (8, 128))

    dx, dy, dz = (of_a(c) - of_b(c) for c in range(3))
    square = dx * dx + dy * dy + dz * dz
    norm_a, norm_b = of_a(3), of_b(3)
    s = square * lax.rsqrt(jnp.maximum(square, 1e-30)) - 0.5
    s_at = jnp.floor(s)
    mu = (MUBINS / 2) * jnp.abs(norm_a - norm_b) * lax.rsqrt(
        jnp.maximum(square, 1.0) * (norm_a + norm_b - square)
    ) - 0.5
    mu_at = jnp.floor(mu)
    both = of_a(4) * of_b(4)
    upper = (mu - mu_at) * both
    return s_at, s - s_at, mu_at, both - upper, upper


def iota(shape, d):
    return lax.broadcasted_iota(i32, shape, d)


def plan(a_weights, b_weights):
    def live(halves):
        count = sum(jnp.where(w > 0.0, 1.0, 0.0) for w in halves)
        return jnp.broadcast_to(jnp.sum(count, axis=1, keepdims=True), count.shape)

    n_a, n_b = live(a_weights), live(b_weights)
    rows_a, rows_b = jnp.ceil(n_a / 8), jnp.ceil(n_b / 8)
    lanes_a, lanes_b = jnp.ceil(n_a / 128), jnp.ceil(n_b / 128)
    turned = jnp.where(rows_b * lanes_a < rows_a * lanes_b, 1.0, 0.0)
    n_lanes = jnp.where(turned > 0.0, lanes_a, lanes_b)
    return turned, n_lanes, jnp.where(turned > 0.0, rows_b, rows_a) * n_lanes


def slot_copy(src, dst, send_sem, recv_sem, device):
    return pltpu.make_async_remote_copy(
        src_ref=src, dst_ref=dst, send_sem=send_sem, recv_sem=recv_sem, device_id=device, device_id_type=MESH
    )


def exchange_kernel(
    n_gx, n_wa, live_ref, count_hbm, list_hbm, pair_hbm, pos_hbm, wgt_hbm, out_ref,
    count_ref, list_ref, pair_ref, pos_ref, wgt_ref, home_ref, stage_ref, own_ref, below_ref, deal_ref,
    load_sems, send_sems, recv_sems,
):
    g, w = lax.axis_index("gx"), lax.axis_index("wa")
    above, under = lax.rem(g + 1, n_gx), lax.rem(g + n_gx - 1, n_gx)
    units = 2 * n_wa
    pairs = ((count_hbm, count_ref), (list_hbm, list_ref), (pair_hbm, pair_ref), (pos_hbm, pos_ref), (wgt_hbm, wgt_ref))
    loads = [pltpu.make_async_copy(src, dst, load_sems.at[k]) for k, (src, dst) in enumerate(pairs)]
    for load in loads:
        load.start()
    barrier = pltpu.get_barrier_semaphore()
    for o in range(n_wa):
        p = lax.rem(w + o, n_wa)
        pl.semaphore_signal(barrier, inc=1, device_id=(under, p), device_id_type=MESH)
        if o:
            pl.semaphore_signal(barrier, inc=1, device_id=(g, p), device_id_type=MESH)
    for load in loads:
        load.wait()

    for b in range(pos_ref.shape[1]):
        for h in range(2):
            at = slice(128 * h, 128 * (h + 1))
            home_ref[b, 4 * h : 4 * h + 3, :] = pos_ref[:, b, at]
            keep = iota((1, 128), 1) + 128 * h < count_ref[b]
            home_ref[b, 4 * h + 3 : 4 * h + 4, :] = jnp.where(keep, wgt_ref[b : b + 1, at], 0.0)
    for q in range(units):
        stage_ref[q] = home_ref[list_ref[0, q % 2, q // 2]]
    pl.semaphore_wait(barrier, 2 * n_wa - 1)

    def two(ref, p):
        return ref.at[pl.ds(2 * p, 2)]

    for o in range(n_wa):
        p = lax.rem(w + o, n_wa)
        slot_copy(two(stage_ref, p), two(below_ref, w), send_sems.at[0], recv_sems.at[0], (above, p)).start()
        if o:
            slot_copy(two(stage_ref, p), two(own_ref, w), send_sems.at[1], recv_sems.at[1], (g, p)).start()
    own_ref[pl.ds(2 * w, 2)] = stage_ref[pl.ds(2 * w, 2)]
    rest = pl.ds(0, units - 2)
    below_all = slot_copy(stage_ref, below_ref, send_sems.at[0], recv_sems.at[0], (above, w))
    own_all = slot_copy(stage_ref.at[rest], own_ref.at[rest], send_sems.at[1], recv_sems.at[1], (above, w))
    below_all.wait_recv()
    own_all.wait_recv()

    active = iota((units, 128), 0) < live_ref[0]
    partner = jnp.concatenate([below_ref[pair_ref[0, u]] for u in range(units)], axis=0)
    row = iota((8 * units, 128), 0)
    dead = ((row & 3) == 3) & ((row >> 3) >= live_ref[0])
    mine = jnp.where(dead, 0.0, own_ref[...].reshape(8 * units, 128))
    three = partner.reshape(units, 8, 128)
    tiles = plan(
        [jnp.where(active, own_ref[:, c, :], 0.0) for c in (3, 7)], [three[:, c, :] for c in (3, 7)]
    )[2]
    unit = iota((units, 128), 0).astype(f32)
    key = tiles * units + (units - 1 - unit)
    on_lanes = jnp.sum(jnp.where(iota((units, 128), 0) == iota((units, 128), 1), key, 0.0), axis=0, keepdims=True)
    more = (on_lanes > key) & (iota((units, 128), 1) < units)
    rank = jnp.sum(jnp.where(more, 1.0, 0.0), axis=1, keepdims=True)
    place = jnp.where(rank < n_wa, rank, (units - 1 + n_wa) - rank)
    wide = (units, 8 * units)
    target = jnp.sum(
        jnp.where(iota(wide, 0) == (iota(wide, 1) >> 3), 8.0 * place + (iota(wide, 1) & 7).astype(f32), 0.0),
        axis=0, keepdims=True,
    )
    square = (8 * units, 8 * units)
    choice = jnp.where(iota(square, 0).astype(f32) == target, 1.0, 0.0).astype(bf16)
    left = jnp.concatenate([mine, partner], axis=1)
    chosen = None
    for _ in range(3):
        part = left.astype(bf16)
        moved = jnp.dot(choice, part, preferred_element_type=f32)
        chosen = moved if chosen is None else chosen + moved
        left = left - part.astype(f32)
    for i in range(units):
        for k in range(2):
            deal_ref[i % n_wa, 2 * (i // n_wa) + k] = chosen[8 * i : 8 * i + 8, 128 * k : 128 * k + 128]

    for o in range(1, n_wa):
        p = lax.rem(w + o, n_wa)
        slot_copy(
            deal_ref.at[o], out_ref.at[pl.ds(4 * w, 4)], send_sems.at[2], recv_sems.at[2], (g, p)
        ).start()
    out_ref[pl.ds(4 * w, 4)] = deal_ref[0]
    below_all.wait_send()
    own_all.wait_send()
    dealt = slot_copy(
        deal_ref.at[pl.ds(1, n_wa - 1)], out_ref.at[pl.ds(0, 4 * (n_wa - 1))], send_sems.at[2], recv_sems.at[2], (above, w)
    )
    dealt.wait_recv()
    dealt.wait_send()


def dealt_blocks(n_gx, n_wa, positions, weights, block_count, send_list, unit_pair, unit_live):
    smem, vmem, anywhere = (pl.BlockSpec(memory_space=m) for m in (pltpu.SMEM, pltpu.VMEM, pl.ANY))
    units = 2 * n_wa
    return pl.pallas_call(
        functools.partial(exchange_kernel, n_gx, n_wa),
        out_shape=pltpu.VMEM((2 * units, 8, 128), f32),
        in_specs=[smem] + [anywhere] * 5,
        out_specs=vmem,
        scratch_shapes=[
            pltpu.SMEM(block_count.shape, i32),
            pltpu.SMEM(send_list.shape, i32),
            pltpu.SMEM(unit_pair.shape, i32),
            pltpu.VMEM(positions.shape, f32),
            pltpu.VMEM(weights.shape, f32),
            pltpu.VMEM((positions.shape[1], 8, 128), f32),
            pltpu.VMEM((units, 8, 128), f32),
            pltpu.VMEM((units, 8, 128), f32),
            pltpu.VMEM((units, 8, 128), f32),
            pltpu.VMEM((n_wa, 4, 8, 128), f32),
            pltpu.SemaphoreType.DMA((5,)),
            pltpu.SemaphoreType.DMA((3,)),
            pltpu.SemaphoreType.DMA((3,)),
        ],
        compiler_params=pltpu.CompilerParams(collective_id=0, has_side_effects=True),
    )(unit_live, block_count, send_list, unit_pair, positions, weights)


def total_kernel(
    n_gx, n_wa, scale, in_ref, slab_out, whole_out, gx_ref, slab_ref, whole_ref, column_ref, send_sems, recv_sems
):
    g, w = lax.axis_index("gx"), lax.axis_index("wa")
    barrier = pltpu.get_barrier_semaphore()
    wa_peers = [lax.rem(w + o, n_wa) for o in range(1, n_wa)]
    gx_peers = [lax.rem(g + o, n_gx) for o in range(1, n_gx)]
    for p in wa_peers:
        pl.semaphore_signal(barrier, inc=1, device_id=(g, p), device_id_type=MESH)
    for p in gx_peers:
        pl.semaphore_signal(barrier, inc=1, device_id=(p, w), device_id_type=MESH)
    pl.semaphore_wait(barrier, n_wa + n_gx - 2)

    for p in gx_peers:
        slot_copy(in_ref, gx_ref.at[g], send_sems.at[0], recv_sems.at[0], (p, w)).start()
    for p in wa_peers:
        slot_copy(in_ref, slab_ref.at[w], send_sems.at[1], recv_sems.at[1], (g, p)).start()
    gx_ref[g] = in_ref[...]
    slab_ref[w] = in_ref[...]

    def all_of(ref, n, k):
        some = ref.at[pl.ds(0, n - 1)]
        return slot_copy(some, some, send_sems.at[k], recv_sems.at[k], (lax.rem(g + 1, n_gx), w))

    all_of(gx_ref, n_gx, 0).wait_recv()
    column = jnp.sum(gx_ref[...], axis=0)
    column_ref[...] = column
    whole_ref[w] = column

    for p in wa_peers:
        slot_copy(column_ref, whole_ref.at[w], send_sems.at[2], recv_sems.at[2], (g, p)).start()
    all_of(slab_ref, n_wa, 1).wait_recv()
    slab_out[...] = jnp.sum(slab_ref[...], axis=0) * scale
    all_of(gx_ref, n_gx, 0).wait_send()
    all_of(slab_ref, n_wa, 1).wait_send()
    all_of(whole_ref, n_wa, 2).wait_recv()
    whole_out[...] = jnp.sum(whole_ref[...], axis=0) * (scale / n_gx)
    all_of(whole_ref, n_wa, 2).wait_send()


def totals(n_gx, n_wa, scale, packed):
    vmem = pl.BlockSpec(memory_space=pltpu.VMEM)
    return pl.pallas_call(
        functools.partial(total_kernel, n_gx, n_wa, scale),
        out_shape=(pltpu.VMEM((8, 128), f32), pltpu.VMEM((8, 128), f32)),
        in_specs=[vmem],
        out_specs=(vmem, vmem),
        scratch_shapes=[
            pltpu.VMEM((n_gx, 8, 128), f32),
            pltpu.VMEM((n_wa, 8, 128), f32),
            pltpu.VMEM((n_wa, 8, 128), f32),
            pltpu.VMEM((8, 128), f32),
            pltpu.SemaphoreType.DMA((3,)),
            pltpu.SemaphoreType.DMA((3,)),
        ],
        compiler_params=pltpu.CompilerParams(collective_id=1, has_side_effects=True),
    )(packed)


def unpack_kernel(slab_ref, whole_ref, slab_out, whole_out):
    for ref, out in ((slab_ref, slab_out.at[:, 0, :]), (whole_ref, whole_out)):
        packed = ref[...]
        for k in range(3):
            rows = min(8, MUBINS - 8 * k)
            turned = packed if k == 0 else pltpu.roll(packed, 128 - 32 * k, 1)
            out[8 * k : 8 * k + rows, :] = turned[:rows, :SBINS]


def unpacked(slab, whole):
    vmem = pl.BlockSpec(memory_space=pltpu.VMEM)
    return pl.pallas_call(
        unpack_kernel,
        out_shape=(
            jax.ShapeDtypeStruct((MUBINS, 1, SBINS), f32),
            jax.ShapeDtypeStruct((MUBINS, SBINS), f32),
        ),
        in_specs=[vmem, vmem],
        out_specs=(vmem, vmem),
    )(slab, whole)


def count_kernel(units, blocks_ref, out_ref, rows_ref, cols_ref, per_unit_ref, list_ref, list_smem, terms_ref, acc_ref, sem):
    n_blocks = 2 * units
    scale = SBINS / reach
    groups = n_blocks // 16

    def weights_of(s):
        return [blocks_ref[pl.ds(s, units, stride=2), 4 * h + 3, :] for h in range(2)]

    turned, n_lanes, tiles = plan(weights_of(0), weights_of(1))
    low = iota((units, units), 1) < iota((units, units), 0)
    start = jnp.dot(jnp.where(low, 1.0, 0.0), tiles, preferred_element_type=f32)
    unit = iota((units, 128), 0).astype(f32)
    eighth = jnp.floor(unit / 8)
    lane16 = 2.0 * (unit - 8.0 * eighth) + turned
    dummy = jnp.float32(2 * n_blocks)
    per_unit_ref[0] = start
    per_unit_ref[1] = start + tiles
    per_unit_ref[2] = jnp.where(n_lanes > 1.5, 0.5, 1.0)
    per_unit_ref[3] = n_lanes
    per_unit_ref[4] = eighth * 65536.0 + lane16 * 256.0 + 2.0 * unit + (1.0 - turned) - dummy
    spot = (iota((8, 128), 0) * 128 + iota((8, 128), 1)).astype(f32)
    n_full = -(-units * 64 // 1024)
    codes = [jnp.full((8, 128), dummy, f32) for _ in range(n_full)]
    for u in range(units):
        first, end, inverse, lanes, base = (jnp.broadcast_to(per_unit_ref[k, u : u + 1, :], (8, 128)) for k in range(5))
        for k in range(n_full):
            place = spot + 1024.0 * k
            at = place - first
            row = jnp.floor(at * inverse)
            code = base + row * 4096.0 + (at - row * lanes) * n_blocks
            code = code + jnp.where(row > 15.5, (groups - 1) * 65536.0, 0.0)
            codes[k] = codes[k] + jnp.where((at >= 0.0) & (place < end), code, 0.0)
    for k in range(n_full):
        list_ref[8 * k : 8 * k + 8, :] = codes[k].astype(i32)
    total = jnp.broadcast_to(jnp.sum(tiles, axis=0, keepdims=True), (8, 128))
    list_ref[8 * n_full : 8 * n_full + 8, :] = jnp.where(iota((8, 128), 0) == 0, dummy, total).astype(i32)
    copy = pltpu.make_async_copy(list_ref, list_smem, sem)
    copy.start()

    at = iota((8, 128), 0)
    eye = sum(jnp.where((at & 3) == c, v, 0.0) for c, v in enumerate(viewer))

    for n in range(n_blocks):
        raw = blocks_ref[n]
        moved = (raw + eye) * scale
        moved = moved * moved
        norm = 2.0 * (moved + pltpu.roll(moved, 7, 0) + pltpu.roll(moved, 6, 0))
        for h in range(2):
            xyz = raw * scale if h == 0 else pltpu.roll(raw * scale, 4, 0)
            weight = pltpu.roll(raw, 1 if h == 0 else 5, 0)
            norms = pltpu.roll(norm, 3 if h == 0 else 7, 0)
            rows_ref[h * n_blocks + n] = jnp.where(at < 3, xyz, jnp.where(at == 3, norms, weight))
    far = 2.0 * sum((v * scale) ** 2 for v in viewer)
    rows_ref[2 * n_blocks] = jnp.where(at == 3, jnp.float32(far), jnp.float32(0.0))
    for k in range(2 * groups):
        cols_ref[k * 128 : (k + 1) * 128, :] = rows_ref[pl.ds(k * 16, 16)].reshape(128, 128).T
    acc_ref[...] = jnp.zeros_like(acc_ref)
    copy.wait()
    trips = (list_smem[8 * n_full + 1, 0] + TILES - 1) // TILES

    def fill(trip):
        for t in range(TILES):
            place = trip * TILES + t
            code = list_smem[place >> 7, place & 127]
            start = pl.multiple_of((code >> 12) * 8, 8)
            terms = tile_terms(cols_ref[pl.ds(start, 8), :], ((code >> 8) & 15) * 8, rows_ref[code & 255])
            for k, v in enumerate(terms):
                terms_ref[t, k] = v

    def both_hats(t):
        s_at, s_part, mu_at, lower, upper = (terms_ref[t, k] for k in range(5))
        return hats(s_at, 1.0 - s_part, s_part, HS), hats(mu_at, lower, upper, HM)

    fill(0)

    def body(trip, carry):
        total = None
        for p in range(TILES // 2):
            s0, m0 = both_hats(2 * p)
            s1, m1 = both_hats(2 * p + 1)
            s = jnp.concatenate([jnp.concatenate(s0, 0), jnp.concatenate(s1, 0)], 1)
            m = jnp.concatenate([jnp.concatenate(m0, 0), jnp.concatenate(m1, 0)], 1)
            r = lax.dot_general(s, m, (((1,), (1,)), ((), ())), preferred_element_type=f32)
            total = r if total is None else total + r
        fill(trip + 1)
        acc_ref[...] += total
        return carry

    lax.fori_loop(0, trips, body, 0)

    sm = (8, 16 * HM)
    same = iota(sm, 0) == (iota(sm, 1) & 7)
    sums = []
    for k in range(SBINS):
        place = 16 * (k % HS) + 8 * (k // HS)
        sums.append(jnp.sum(jnp.where(same, acc_ref[place : place + 8, :], 0.0), axis=0, keepdims=True))
    by_s = jnp.concatenate(sums + [jnp.zeros((128 - SBINS, 16 * HM), f32)], axis=0)
    r, c = iota((32, 16 * HM), 0), iota((32, 16 * HM), 1)
    to_m = jnp.where((c >> 4) + HM * ((c >> 3) & 1) == r, 1.0, 0.0)
    bins = lax.dot_general(
        to_m, by_s, (((1,), (1,)), ((), ())), precision=lax.Precision.HIGHEST, preferred_element_type=f32
    )
    packed = bins[0:8]
    for k in range(1, 3):
        packed = packed + pltpu.roll(bins[8 * k : 8 * k + 8], 32 * k, 1)
    out_ref[...] = packed


def pair_counts(blocks):
    units = blocks.shape[0] // 2
    n_list = 8 * (-(-units * 64 // 1024) + 1)
    return pl.pallas_call(
        functools.partial(count_kernel, units),
        out_shape=pltpu.VMEM((8, 128), f32),
        in_specs=[pl.BlockSpec(memory_space=pltpu.VMEM)],
        out_specs=pl.BlockSpec(memory_space=pltpu.VMEM),
        scratch_shapes=[
            pltpu.VMEM((4 * units + 1, 8, 128), f32),
            pltpu.VMEM((2 * (units // 8) * 128, 128), f32),
            pltpu.VMEM((5, units, 128), f32),
            pltpu.VMEM((n_list, 128), i32),
            pltpu.SMEM((n_list, 128), i32),
            pltpu.VMEM((TILES, 5, 8, 128), f32),
            pltpu.VMEM((16 * HS, 16 * HM), f32),
            pltpu.SemaphoreType.DMA,
        ],
    )(blocks)


def in_vmem(x):
    return pltpu.with_memory_space_constraint(x, pltpu.VMEM)


def solution(mesh):
    n_gx, n_wa = mesh.shape["gx"], mesh.shape["wa"]
    units = 2 * n_wa
    scale = 10.0 * SBINS * MUBINS / (n_wa * units * 256 * 256)

    def per_device(positions, weights, block_count, send_list, unit_pair, unit_live):
        dealt = dealt_blocks(
            n_gx, n_wa, jnp.transpose(positions, (1, 0, 2)), weights, block_count,
            jnp.transpose(send_list, (0, 2, 1)), unit_pair, unit_live,
        )
        packed = pair_counts(in_vmem(dealt))
        slab, whole = totals(n_gx, n_wa, scale, in_vmem(packed))
        slab, whole = unpacked(in_vmem(slab), in_vmem(whole))
        return jnp.transpose(slab, (1, 2, 0)), whole.T

    return jax.shard_map(
        per_device,
        mesh=mesh,
        in_specs=(P(("gx", "wa")),) * 6,
        out_specs=(P("gx", None, None), P()),
        check_vma=False,
    )
```

```python
import functools

import jax
import jax.numpy as jnp
from jax import lax
from jax.experimental import pallas as pl
from jax.experimental.pallas import tpu as pltpu
from jax.sharding import PartitionSpec as P

SBINS = 30
MUBINS = 20
HS, HM = SBINS // 2, MUBINS // 2
reach = 0.5
viewer = (0.5, 0.5, -1.5)
TILES = 48
f32, bf16, i32 = jnp.float32, jnp.bfloat16, jnp.int32
MESH = pl.DeviceIdType.MESH


def hats(at, first, second, half):
    spot = jnp.concatenate([at, at - half], axis=0).astype(bf16)
    first = jnp.concatenate([first, first], axis=0).astype(bf16)
    second = jnp.concatenate([second, second], axis=0).astype(bf16)
    zero = jnp.zeros_like(first)
    before = spot == jnp.asarray(-1, bf16)
    out = []
    for q in range(half):
        here = spot == jnp.asarray(q, bf16)
        out.append(jnp.where(here, first, jnp.where(before, second, zero)))
        before = here
    return out


def lane_pick(x, lane):
    numbers = lax.GatherDimensionNumbers(
        offset_dims=(), collapsed_slice_dims=(1,), start_index_map=(1,), operand_batching_dims=(0,), start_indices_batching_dims=(0,)
    )
    return lax.gather(x, lane[..., None], numbers, slice_sizes=(1, 1), mode=lax.GatherScatterMode.PROMISE_IN_BOUNDS)


def tile_terms(cols, lane_at, row):
    def of_a(c):
        return lane_pick(cols, jnp.full((8, 128), lane_at + c, i32))

    def of_b(c):
        return jnp.broadcast_to(row[c : c + 1, :], (8, 128))

    dx, dy, dz = (of_a(c) - of_b(c) for c in range(3))
    square = dx * dx + dy * dy + dz * dz
    norm_a, norm_b = of_a(3), of_b(3)
    s = square * lax.rsqrt(jnp.maximum(square, 1e-30)) - 0.5
    s_at = jnp.floor(s)
    mu = (MUBINS / 2) * jnp.abs(norm_a - norm_b) * lax.rsqrt(
        jnp.maximum(square, 1.0) * (norm_a + norm_b - square)
    ) - 0.5
    mu_at = jnp.floor(mu)
    both = of_a(4) * of_b(4)
    upper = (mu - mu_at) * both
    return s_at, s - s_at, mu_at, both - upper, upper


def iota(shape, d):
    return lax.broadcasted_iota(i32, shape, d)


def plan(a_weights, b_weights):
    def live(halves):
        count = sum(jnp.where(w > 0.0, 1.0, 0.0) for w in halves)
        return jnp.broadcast_to(jnp.sum(count, axis=1, keepdims=True), count.shape)

    n_a, n_b = live(a_weights), live(b_weights)
    rows_a, rows_b = jnp.ceil(n_a / 8), jnp.ceil(n_b / 8)
    lanes_a, lanes_b = jnp.ceil(n_a / 128), jnp.ceil(n_b / 128)
    turned = jnp.where(rows_b * lanes_a < rows_a * lanes_b, 1.0, 0.0)
    n_lanes = jnp.where(turned > 0.0, lanes_a, lanes_b)
    return turned, n_lanes, jnp.where(turned > 0.0, rows_b, rows_a) * n_lanes


def slot_copy(src, dst, send_sem, recv_sem, device):
    return pltpu.make_async_remote_copy(
        src_ref=src, dst_ref=dst, send_sem=send_sem, recv_sem=recv_sem, device_id=device, device_id_type=MESH
    )


def exchange_kernel(
    n_gx, n_wa, live_ref, count_hbm, list_hbm, pair_hbm, pos_hbm, wgt_hbm, out_ref,
    count_ref, list_ref, pair_ref, pos_ref, wgt_ref, home_ref, stage_ref, own_ref, below_ref, deal_ref,
    load_sems, send_sems, recv_sems,
):
    g, w = lax.axis_index("gx"), lax.axis_index("wa")
    above, under = lax.rem(g + 1, n_gx), lax.rem(g + n_gx - 1, n_gx)
    units = 2 * n_wa
    pairs = ((count_hbm, count_ref), (list_hbm, list_ref), (pair_hbm, pair_ref), (pos_hbm, pos_ref), (wgt_hbm, wgt_ref))
    loads = [pltpu.make_async_copy(src, dst, load_sems.at[k]) for k, (src, dst) in enumerate(pairs)]
    for load in loads:
        load.start()
    barrier = pltpu.get_barrier_semaphore()
    for o in range(n_wa):
        p = lax.rem(w + o, n_wa)
        pl.semaphore_signal(barrier, inc=1, device_id=(under, p), device_id_type=MESH)
        if o:
            pl.semaphore_signal(barrier, inc=1, device_id=(g, p), device_id_type=MESH)
    for load in loads:
        load.wait()

    for b in range(pos_ref.shape[1]):
        for h in range(2):
            at = slice(128 * h, 128 * (h + 1))
            home_ref[b, 4 * h : 4 * h + 3, :] = pos_ref[:, b, at]
            keep = iota((1, 128), 1) + 128 * h < count_ref[b]
            home_ref[b, 4 * h + 3 : 4 * h + 4, :] = jnp.where(keep, wgt_ref[b : b + 1, at], 0.0)
    for q in range(units):
        stage_ref[q] = home_ref[list_ref[0, q % 2, q // 2]]
    pl.semaphore_wait(barrier, 2 * n_wa - 1)

    def two(ref, p):
        return ref.at[pl.ds(2 * p, 2)]

    for o in range(n_wa):
        p = lax.rem(w + o, n_wa)
        slot_copy(two(stage_ref, p), two(below_ref, w), send_sems.at[0], recv_sems.at[0], (above, p)).start()
        if o:
            slot_copy(two(stage_ref, p), two(own_ref, w), send_sems.at[1], recv_sems.at[1], (g, p)).start()
    own_ref[pl.ds(2 * w, 2)] = stage_ref[pl.ds(2 * w, 2)]
    rest = pl.ds(0, units - 2)
    below_all = slot_copy(stage_ref, below_ref, send_sems.at[0], recv_sems.at[0], (above, w))
    own_all = slot_copy(stage_ref.at[rest], own_ref.at[rest], send_sems.at[1], recv_sems.at[1], (above, w))
    below_all.wait_recv()
    own_all.wait_recv()

    active = iota((units, 128), 0) < live_ref[0]
    partner = jnp.concatenate([below_ref[pair_ref[0, u]] for u in range(units)], axis=0)
    row = iota((8 * units, 128), 0)
    dead = ((row & 3) == 3) & ((row >> 3) >= live_ref[0])
    mine = jnp.where(dead, 0.0, own_ref[...].reshape(8 * units, 128))
    three = partner.reshape(units, 8, 128)
    tiles = plan(
        [jnp.where(active, own_ref[:, c, :], 0.0) for c in (3, 7)], [three[:, c, :] for c in (3, 7)]
    )[2]
    unit = iota((units, 128), 0).astype(f32)
    key = tiles * units + (units - 1 - unit)
    wide = (units, 8 * units)
    key = jnp.concatenate([key] * -(-8 * units // 128), axis=1)[:, : 8 * units]
    on_lanes = jnp.sum(jnp.where(iota(wide, 0) == (iota(wide, 1) >> 3), key, 0.0), axis=0, keepdims=True)
    rank = jnp.sum(jnp.where(key > on_lanes, 1.0, 0.0), axis=0, keepdims=True)
    place = jnp.where(rank < n_wa, rank, (units - 1 + n_wa) - rank)
    target = 8.0 * place + (iota((1, 8 * units), 1) & 7).astype(f32)
    square = (8 * units, 8 * units)
    choice = jnp.where(iota(square, 0).astype(f32) == target, 1.0, 0.0).astype(bf16)
    left = jnp.concatenate([mine, partner], axis=1)
    chosen = None
    for _ in range(3):
        part = left.astype(bf16)
        moved = jnp.dot(choice, part, preferred_element_type=f32)
        chosen = moved if chosen is None else chosen + moved
        left = left - part.astype(f32)
    for i in range(units):
        for k in range(2):
            deal_ref[i % n_wa, 2 * (i // n_wa) + k] = chosen[8 * i : 8 * i + 8, 128 * k : 128 * k + 128]

    for o in range(1, n_wa):
        p = lax.rem(w + o, n_wa)
        slot_copy(
            deal_ref.at[o], out_ref.at[pl.ds(4 * w, 4)], send_sems.at[2], recv_sems.at[2], (g, p)
        ).start()
    out_ref[pl.ds(4 * w, 4)] = deal_ref[0]
    below_all.wait_send()
    own_all.wait_send()
    dealt = slot_copy(
        deal_ref.at[pl.ds(1, n_wa - 1)], out_ref.at[pl.ds(0, 4 * (n_wa - 1))], send_sems.at[2], recv_sems.at[2], (above, w)
    )
    dealt.wait_recv()
    dealt.wait_send()


def dealt_blocks(n_gx, n_wa, positions, weights, block_count, send_list, unit_pair, unit_live):
    smem, vmem, anywhere = (pl.BlockSpec(memory_space=m) for m in (pltpu.SMEM, pltpu.VMEM, pl.ANY))
    units = 2 * n_wa
    return pl.pallas_call(
        functools.partial(exchange_kernel, n_gx, n_wa),
        out_shape=pltpu.VMEM((2 * units, 8, 128), f32),
        in_specs=[smem] + [anywhere] * 5,
        out_specs=vmem,
        scratch_shapes=[
            pltpu.SMEM(block_count.shape, i32),
            pltpu.SMEM(send_list.shape, i32),
            pltpu.SMEM(unit_pair.shape, i32),
            pltpu.VMEM(positions.shape, f32),
            pltpu.VMEM(weights.shape, f32),
            pltpu.VMEM((positions.shape[1], 8, 128), f32),
            pltpu.VMEM((units, 8, 128), f32),
            pltpu.VMEM((units, 8, 128), f32),
            pltpu.VMEM((units, 8, 128), f32),
            pltpu.VMEM((n_wa, 4, 8, 128), f32),
            pltpu.SemaphoreType.DMA((5,)),
            pltpu.SemaphoreType.DMA((3,)),
            pltpu.SemaphoreType.DMA((3,)),
        ],
        compiler_params=pltpu.CompilerParams(collective_id=0, has_side_effects=True),
    )(unit_live, block_count, send_list, unit_pair, positions, weights)


def total_kernel(
    n_gx, n_wa, scale, in_ref, slab_out, whole_out, gx_ref, slab_ref, whole_ref, column_ref, send_sems, recv_sems
):
    g, w = lax.axis_index("gx"), lax.axis_index("wa")
    barrier = pltpu.get_barrier_semaphore()
    wa_peers = [lax.rem(w + o, n_wa) for o in range(1, n_wa)]
    gx_peers = [lax.rem(g + o, n_gx) for o in range(1, n_gx)]
    for p in gx_peers:
        pl.semaphore_signal(barrier, inc=1, device_id=(p, w), device_id_type=MESH)
    for p in wa_peers:
        pl.semaphore_signal(barrier, inc=1, device_id=(g, p), device_id_type=MESH)
    pl.semaphore_wait(barrier, n_wa + n_gx - 2)

    for p in gx_peers:
        slot_copy(in_ref, gx_ref.at[g], send_sems.at[0], recv_sems.at[0], (p, w)).start()
    for p in wa_peers:
        slot_copy(in_ref, slab_ref.at[w], send_sems.at[1], recv_sems.at[1], (g, p)).start()
    gx_ref[g] = in_ref[...]
    slab_ref[w] = in_ref[...]

    def all_of(ref, n, k):
        some = ref.at[pl.ds(0, n - 1)]
        return slot_copy(some, some, send_sems.at[k], recv_sems.at[k], (lax.rem(g + 1, n_gx), w))

    all_of(gx_ref, n_gx, 0).wait_recv()
    column = jnp.sum(gx_ref[...], axis=0)
    column_ref[...] = column
    whole_ref[w] = column

    for p in wa_peers:
        slot_copy(column_ref, whole_ref.at[w], send_sems.at[2], recv_sems.at[2], (g, p)).start()
    all_of(slab_ref, n_wa, 1).wait_recv()
    slab_out[...] = jnp.sum(slab_ref[...], axis=0) * scale
    all_of(gx_ref, n_gx, 0).wait_send()
    all_of(slab_ref, n_wa, 1).wait_send()
    all_of(whole_ref, n_wa, 2).wait_recv()
    whole_out[...] = jnp.sum(whole_ref[...], axis=0) * (scale / n_gx)
    all_of(whole_ref, n_wa, 2).wait_send()


def totals(n_gx, n_wa, scale, packed):
    vmem = pl.BlockSpec(memory_space=pltpu.VMEM)
    return pl.pallas_call(
        functools.partial(total_kernel, n_gx, n_wa, scale),
        out_shape=(pltpu.VMEM((8, 128), f32), pltpu.VMEM((8, 128), f32)),
        in_specs=[vmem],
        out_specs=(vmem, vmem),
        scratch_shapes=[
            pltpu.VMEM((n_gx, 8, 128), f32),
            pltpu.VMEM((n_wa, 8, 128), f32),
            pltpu.VMEM((n_wa, 8, 128), f32),
            pltpu.VMEM((8, 128), f32),
            pltpu.SemaphoreType.DMA((3,)),
            pltpu.SemaphoreType.DMA((3,)),
        ],
        compiler_params=pltpu.CompilerParams(collective_id=1, has_side_effects=True),
    )(packed)


def unpack_kernel(slab_ref, whole_ref, slab_out, whole_out):
    for ref, out in ((slab_ref, slab_out.at[:, 0, :]), (whole_ref, whole_out)):
        packed = ref[...]
        for k in range(3):
            rows = min(8, MUBINS - 8 * k)
            turned = packed if k == 0 else pltpu.roll(packed, 128 - 32 * k, 1)
            out[8 * k : 8 * k + rows, :] = turned[:rows, :SBINS]


def unpacked(slab, whole):
    vmem = pl.BlockSpec(memory_space=pltpu.VMEM)
    return pl.pallas_call(
        unpack_kernel,
        out_shape=(
            jax.ShapeDtypeStruct((MUBINS, 1, SBINS), f32),
            jax.ShapeDtypeStruct((MUBINS, SBINS), f32),
        ),
        in_specs=[vmem, vmem],
        out_specs=(vmem, vmem),
    )(slab, whole)


def count_kernel(units, blocks_ref, out_ref, rows_ref, cols_ref, per_unit_ref, list_ref, list_smem, terms_ref, acc_ref, sem):
    n_blocks = 2 * units
    scale = SBINS / reach
    groups = n_blocks // 16

    def weights_of(s):
        return [blocks_ref[pl.ds(s, units, stride=2), 4 * h + 3, :] for h in range(2)]

    turned, n_lanes, tiles = plan(weights_of(0), weights_of(1))
    start, step = tiles, 1
    while step < units:
        start = start + jnp.where(iota((units, 128), 0) >= step, pltpu.roll(start, step, 0), 0.0)
        step *= 2
    start = start - tiles
    unit = iota((units, 128), 0).astype(f32)
    eighth = jnp.floor(unit / 8)
    lane16 = 2.0 * (unit - 8.0 * eighth) + turned
    dummy = jnp.float32(2 * n_blocks)
    per_unit_ref[0] = start
    per_unit_ref[1] = start + tiles
    per_unit_ref[2] = jnp.where(n_lanes > 1.5, 0.5, 1.0)
    per_unit_ref[3] = n_lanes
    per_unit_ref[4] = eighth * 65536.0 + lane16 * 256.0 + 2.0 * unit + (1.0 - turned) - dummy
    spot = (iota((8, 128), 0) * 128 + iota((8, 128), 1)).astype(f32)
    n_full = -(-units * 64 // 1024)
    codes = [jnp.full((8, 128), dummy, f32) for _ in range(n_full)]
    for u in range(units):
        first, end, inverse, lanes, base = (jnp.broadcast_to(per_unit_ref[k, u : u + 1, :], (8, 128)) for k in range(5))
        for k in range(n_full):
            place = spot + 1024.0 * k
            at = place - first
            row = jnp.floor(at * inverse)
            code = base + row * 4096.0 + (at - row * lanes) * n_blocks
            code = code + jnp.where(row > 15.5, (groups - 1) * 65536.0, 0.0)
            codes[k] = codes[k] + jnp.where((at >= 0.0) & (place < end), code, 0.0)
    for k in range(n_full):
        list_ref[8 * k : 8 * k + 8, :] = codes[k].astype(i32)
    total = jnp.broadcast_to(jnp.sum(tiles, axis=0, keepdims=True), (8, 128))
    list_ref[8 * n_full : 8 * n_full + 8, :] = jnp.where(iota((8, 128), 0) == 0, dummy, total).astype(i32)
    copy = pltpu.make_async_copy(list_ref, list_smem, sem)
    copy.start()

    at = iota((8, 128), 0)
    eye = sum(jnp.where((at & 3) == c, v, 0.0) for c, v in enumerate(viewer))

    share = max(1, groups // 2)

    def prepare(turn, carry):
        for i in range(16 * share):
            n = turn * (16 * share) + i
            raw = blocks_ref[n]
            moved = (raw + eye) * scale
            moved = moved * moved
            norm = 2.0 * (moved + pltpu.roll(moved, 7, 0) + pltpu.roll(moved, 6, 0))
            for h in range(2):
                xyz = raw * scale if h == 0 else pltpu.roll(raw * scale, 4, 0)
                weight = pltpu.roll(raw, 1 if h == 0 else 5, 0)
                norms = pltpu.roll(norm, 3 if h == 0 else 7, 0)
                rows_ref[h * n_blocks + n] = jnp.where(at < 3, xyz, jnp.where(at == 3, norms, weight))
        for h in range(2):
            for k in range(share):
                group = h * groups + turn * share + k
                place = pl.multiple_of(group * 128, 128)
                cols_ref[pl.ds(place, 128), :] = rows_ref[pl.ds(group * 16, 16)].reshape(128, 128).T
        return carry

    lax.fori_loop(0, groups // share, prepare, 0)
    far = 2.0 * sum((v * scale) ** 2 for v in viewer)
    rows_ref[2 * n_blocks] = jnp.where(at == 3, jnp.float32(far), jnp.float32(0.0))
    acc_ref[...] = jnp.zeros_like(acc_ref)
    copy.wait()
    trips = (list_smem[8 * n_full + 1, 0] + TILES - 1) // TILES

    def fill(trip):
        for t in range(TILES):
            place = trip * TILES + t
            code = list_smem[place >> 7, place & 127]
            start = pl.multiple_of((code >> 12) * 8, 8)
            terms = tile_terms(cols_ref[pl.ds(start, 8), :], ((code >> 8) & 15) * 8, rows_ref[code & 255])
            for k, v in enumerate(terms):
                terms_ref[t, k] = v

    def both_hats(t):
        s_at, s_part, mu_at, lower, upper = (terms_ref[t, k] for k in range(5))
        return hats(s_at, 1.0 - s_part, s_part, HS), hats(mu_at, lower, upper, HM)

    fill(0)

    def body(trip, carry):
        total = None
        for p in range(TILES // 2):
            s0, m0 = both_hats(2 * p)
            s1, m1 = both_hats(2 * p + 1)
            s = jnp.concatenate([jnp.concatenate(s0, 0), jnp.concatenate(s1, 0)], 1)
            m = jnp.concatenate([jnp.concatenate(m0, 0), jnp.concatenate(m1, 0)], 1)
            r = lax.dot_general(s, m, (((1,), (1,)), ((), ())), preferred_element_type=f32)
            total = r if total is None else total + r
        fill(trip + 1)
        acc_ref[...] += total
        return carry

    lax.fori_loop(0, trips, body, 0)

    sm = (8, 16 * HM)
    same = iota(sm, 0) == (iota(sm, 1) & 7)
    sums = []
    for k in range(SBINS):
        place = 16 * (k % HS) + 8 * (k // HS)
        sums.append(jnp.sum(jnp.where(same, acc_ref[place : place + 8, :], 0.0), axis=0, keepdims=True))
    by_s = jnp.concatenate(sums + [jnp.zeros((128 - SBINS, 16 * HM), f32)], axis=0)
    r, c = iota((32, 16 * HM), 0), iota((32, 16 * HM), 1)
    to_m = jnp.where((c >> 4) + HM * ((c >> 3) & 1) == r, 1.0, 0.0)
    bins = lax.dot_general(
        to_m, by_s, (((1,), (1,)), ((), ())), precision=lax.Precision.HIGHEST, preferred_element_type=f32
    )
    packed = bins[0:8]
    for k in range(1, 3):
        packed = packed + pltpu.roll(bins[8 * k : 8 * k + 8], 32 * k, 1)
    out_ref[...] = packed


def pair_counts(blocks):
    units = blocks.shape[0] // 2
    n_list = 8 * (-(-units * 64 // 1024) + 1)
    return pl.pallas_call(
        functools.partial(count_kernel, units),
        out_shape=pltpu.VMEM((8, 128), f32),
        in_specs=[pl.BlockSpec(memory_space=pltpu.VMEM)],
        out_specs=pl.BlockSpec(memory_space=pltpu.VMEM),
        scratch_shapes=[
            pltpu.VMEM((4 * units + 1, 8, 128), f32),
            pltpu.VMEM((2 * (units // 8) * 128, 128), f32),
            pltpu.VMEM((5, units, 128), f32),
            pltpu.VMEM((n_list, 128), i32),
            pltpu.SMEM((n_list, 128), i32),
            pltpu.VMEM((TILES, 5, 8, 128), f32),
            pltpu.VMEM((16 * HS, 16 * HM), f32),
            pltpu.SemaphoreType.DMA,
        ],
    )(blocks)


def in_vmem(x):
    return pltpu.with_memory_space_constraint(x, pltpu.VMEM)


def solution(mesh):
    n_gx, n_wa = mesh.shape["gx"], mesh.shape["wa"]
    units = 2 * n_wa
    scale = 10.0 * SBINS * MUBINS / (n_wa * units * 256 * 256)

    def per_device(positions, weights, block_count, send_list, unit_pair, unit_live):
        dealt = dealt_blocks(
            n_gx, n_wa, jnp.transpose(positions, (1, 0, 2)), weights, block_count,
            jnp.transpose(send_list, (0, 2, 1)), unit_pair, unit_live,
        )
        packed = pair_counts(in_vmem(dealt))
        slab, whole = totals(n_gx, n_wa, scale, in_vmem(packed))
        slab, whole = unpacked(in_vmem(slab), in_vmem(whole))
        return jnp.transpose(slab, (1, 2, 0)), whole.T

    return jax.shard_map(
        per_device,
        mesh=mesh,
        in_specs=(P(("gx", "wa")),) * 6,
        out_specs=(P("gx", None, None), P()),
        check_vma=False,
    )
```
